32 devices in a mesh: dp: 32 (over z, y, x, core).
Axes of the slice: x: 2, y: 2, z: 4, core: 2. Of those that a mesh axis runs over, the one named last changes fastest.
Arguments:
- tokens_in: bfloat16 [16384, 1024], P('dp')
- w_one: bfloat16 [1024, 4096], replicated
- w_two: bfloat16 [4096, 1024], replicated
- item_table: bfloat16 [131072, 1024], P('dp')
- cand_ids: int32 [4096], replicated
- cand_logq: float32 [4096], replicated
- targets: int32 [16384], P('dp')
Outputs:
- output 1: float32 [], replicated
- output 2: float32 [131072, 1024], P('dp')
- output 3: float32 [1024, 4096], replicated
- output 4: float32 [4096, 1024], replicated
All inputs are finite; a program needn't handle non-finite values.
Results may differ from the reference program's by a relative error of at most 0.00824958.
Values are sent between devices in bfloat16 or wider.
A program may use at most 1 GiB of HBM per device.

```python
import jax
import jax.numpy as jnp
from jax import lax

TOKENS = 16384
ROW_BLOCK = 1024
IN_DIM = 1024
HIDDEN = 4096
EMBED_DIM = 1024
TABLE_ROWS = 131072
NUM_CANDS = 4096
HOT_ROWS = TABLE_ROWS // 8
HALF_CANDS = NUM_CANDS // 2


def setup_inputs(seed: int = 0) -> dict:
    keys = jax.random.split(jax.random.key(seed), 12)
    tokens_in = jax.random.normal(keys[0], (TOKENS, IN_DIM), jnp.float32).astype(jnp.bfloat16)
    w_one = (jax.random.normal(keys[1], (IN_DIM, HIDDEN), jnp.float32) * IN_DIM ** -0.5).astype(jnp.bfloat16)
    w_two = (jax.random.normal(keys[2], (HIDDEN, EMBED_DIM), jnp.float32) * HIDDEN ** -0.5).astype(jnp.bfloat16)
    item_table = (jax.random.normal(keys[3], (TABLE_ROWS, EMBED_DIM), jnp.float32) * (3.0 * EMBED_DIM ** -0.5)).astype(jnp.bfloat16)
    hot_ids = jax.random.permutation(keys[4], HOT_ROWS)[:HALF_CANDS]
    tail_ids = HOT_ROWS + jax.random.permutation(keys[5], TABLE_ROWS - HOT_ROWS)[:NUM_CANDS - HALF_CANDS]
    hot_logq = jax.random.uniform(keys[6], (HALF_CANDS,), jnp.float32, -1.0, 1.5)
    tail_logq = jax.random.uniform(keys[7], (NUM_CANDS - HALF_CANDS,), jnp.float32, -3.5, -1.0)
    cand_order = jax.random.permutation(keys[8], NUM_CANDS)
    cand_ids = jnp.concatenate([hot_ids, tail_ids]).astype(jnp.int32)[cand_order]
    cand_logq = jnp.concatenate([hot_logq, tail_logq])[cand_order]
    hit_flag = jax.random.randint(keys[9], (TOKENS,), 0, 2)
    hit_pick = jax.random.randint(keys[10], (TOKENS,), 0, NUM_CANDS)
    free_ids = jax.random.randint(keys[11], (TOKENS,), 0, TABLE_ROWS)
    targets = jnp.where(hit_flag == 1, cand_ids[hit_pick], free_ids).astype(jnp.int32)
    return {'tokens_in': tokens_in, 'w_one': w_one, 'w_two': w_two, 'item_table': item_table,
            'cand_ids': cand_ids, 'cand_logq': cand_logq, 'targets': targets}


def reference(tokens_in, w_one, w_two, item_table, cand_ids, cand_logq, targets):
    cand_rows = item_table[cand_ids].astype(jnp.float32)
    n_blocks = TOKENS // ROW_BLOCK
    x_blocks = tokens_in.reshape(n_blocks, ROW_BLOCK, IN_DIM)
    y_blocks = targets.reshape(n_blocks, ROW_BLOCK)
    w_two_f = w_two.astype(jnp.float32)

    def block_step(carry_in, inputs):
        loss_acc, cand_grad, grad_one, grad_two = carry_in
        x_blk, y_blk = inputs
        pre_act = jnp.dot(x_blk, w_one, preferred_element_type=jnp.float32).astype(jnp.bfloat16)
        act_val, gelu_back = jax.vjp(jax.nn.gelu, pre_act.astype(jnp.float32))
        hidden_act = act_val.astype(jnp.bfloat16).astype(jnp.float32)
        query_vec = jnp.dot(hidden_act, w_two_f).astype(jnp.bfloat16).astype(jnp.float32)
        tgt_rows = item_table[y_blk].astype(jnp.float32)
        z_tgt = jnp.sum(query_vec * tgt_rows, axis=1)
        z_cand = jnp.dot(query_vec, cand_rows.T) - cand_logq[None, :]
        z_cand = jnp.where(y_blk[:, None] == cand_ids[None, :], -1e9, z_cand)
        peak_val = jnp.maximum(jnp.max(z_cand, axis=1), z_tgt)
        exp_total = jnp.exp(z_tgt - peak_val) + jnp.sum(jnp.exp(z_cand - peak_val[:, None]), axis=1)
        log_norm = peak_val + jnp.log(exp_total)
        loss_acc = loss_acc + jnp.sum(log_norm - z_tgt)
        dz_tgt = (jnp.exp(z_tgt - log_norm) - 1.0) / TOKENS
        dz_cand = (jnp.exp(z_cand - log_norm[:, None]) / TOKENS).astype(jnp.bfloat16).astype(jnp.float32)
        d_query = (dz_tgt[:, None] * tgt_rows + jnp.dot(dz_cand, cand_rows)).astype(jnp.bfloat16).astype(jnp.float32)
        cand_grad = cand_grad + jnp.dot(dz_cand.T, query_vec)
        grad_two = grad_two + jnp.dot(hidden_act.T, d_query)
        d_act = jnp.dot(d_query, w_two_f.T).astype(jnp.bfloat16).astype(jnp.float32)
        d_pre = gelu_back(d_act)[0].astype(jnp.bfloat16).astype(jnp.float32)
        grad_one = grad_one + jnp.dot(x_blk.astype(jnp.float32).T, d_pre)
        return (loss_acc, cand_grad, grad_one, grad_two), dz_tgt[:, None] * query_vec

    init_carry = (jnp.zeros((), jnp.float32), jnp.zeros((NUM_CANDS, EMBED_DIM), jnp.float32),
                  jnp.zeros((IN_DIM, HIDDEN), jnp.float32), jnp.zeros((HIDDEN, EMBED_DIM), jnp.float32))
    final_carry, tgt_grads = lax.scan(block_step, init_carry, (x_blocks, y_blocks))
    loss_acc, cand_grad, grad_one, grad_two = final_carry
    grad_table = jnp.zeros((TABLE_ROWS, EMBED_DIM), jnp.float32).at[cand_ids].add(cand_grad)
    grad_table = grad_table.at[targets].add(tgt_grads.reshape(TOKENS, EMBED_DIM))
    return loss_acc / TOKENS, grad_table, grad_one, grad_two
```

```python
import functools

import jax
import jax.numpy as jnp
from jax import lax
from jax.experimental import pallas as pl
from jax.experimental.pallas import tpu as pltpu
from jax.sharding import PartitionSpec as P

MESH = pl.DeviceIdType.MESH
PARTS = 8


def spread_kernel(n, in_ref, out_ref, send_sem, recv_sem):
    me = lax.axis_index('dp')
    barrier = pltpu.get_barrier_semaphore()

    def greet(i, carry):
        pl.semaphore_signal(barrier, inc=1, device_id=(lax.rem(me + i, n),), device_id_type=MESH)
        return carry

    lax.fori_loop(1, n, greet, 0)
    pl.semaphore_wait(barrier, n - 1)

    def send(i, carry):
        pltpu.make_async_remote_copy(
            src_ref=in_ref, dst_ref=out_ref.at[me], send_sem=send_sem, recv_sem=recv_sem,
            device_id=(lax.rem(me + i, n),), device_id_type=MESH).start()
        return carry

    lax.fori_loop(1, n, send, 0)
    others = out_ref.at[pl.ds(0, n - 1)]
    drain = pltpu.make_async_remote_copy(
        src_ref=others, dst_ref=others, send_sem=send_sem, recv_sem=recv_sem,
        device_id=(me,), device_id_type=MESH)
    drain.wait_recv()
    drain.wait_send()
    out_ref[me] = in_ref[...]


def spread(block, n, cid):
    return pl.pallas_call(
        functools.partial(spread_kernel, n),
        out_shape=jax.ShapeDtypeStruct((n,) + block.shape, block.dtype),
        in_specs=[pl.BlockSpec(memory_space=pltpu.VMEM)],
        out_specs=pl.BlockSpec(memory_space=pltpu.VMEM),
        scratch_shapes=[pltpu.SemaphoreType.DMA, pltpu.SemaphoreType.DMA],
        compiler_params=pltpu.CompilerParams(collective_id=cid, has_side_effects=True),
        name=f'spread_{cid}',
    )(block)


def reduce_kernel(tile, steps, in_ref, out_ref, acc, *scratch):
    got, (load_sem, send_sem, recv_sem, store_sem) = scratch[:steps], scratch[steps:]
    me = lax.axis_index('dp')
    core = lax.rem(me, 2)
    xb, yb = lax.rem(me // 2, 2), lax.rem(me // 4, 2)
    z0, z1 = lax.rem(me // 8, 2), lax.rem(me // 16, 2)
    w1, w2 = 1 + core, 2 - core
    b1 = xb * (1 - core) + yb * core
    b2 = yb * (1 - core) + xb * core
    bits = (core, b1, b2, z0, z1)
    mates = [me + 2 * w * (1 - 2 * b) for b, w in zip(bits[1:], (w1, w2, 4, 8))]
    mates = ([me + 1 - 2 * core] + mates)[:steps]
    barrier = pltpu.get_barrier_semaphore()
    for mate in mates:
        pl.semaphore_signal(barrier, inc=1, device_id=(mate,), device_id_type=MESH)

    def piece(part):
        if tile[0] is None:
            return (slice(None), pl.ds(part * tile[1], tile[1]))
        return (pl.ds(part * tile[0], tile[0]),)

    def load(part):
        return pltpu.make_async_copy(in_ref.at[(slice(None), core) + piece(part)], acc.at[part], load_sem.at[part])

    for part in range(PARTS):
        load(part).start()
    pl.semaphore_wait(barrier, steps)

    def place(step, i, bit):
        if step == 1:
            return bit * w1 + lax.rem(i, 2) * w2 + (i // 2) * 4
        base = b1 * w1
        if step == 2:
            return base + bit * w2 + i * 4
        base = base + b2 * w2
        if step == 3:
            return base + bit * 4 + i * 8
        return base + z0 * 4 + bit * 8

    def send(step, part):
        if step == 0:
            pltpu.make_async_remote_copy(
                src_ref=in_ref.at[(slice(None), 1 - core) + piece(part)], dst_ref=got[0].at[part],
                send_sem=send_sem.at[0, part], recv_sem=recv_sem.at[0, part],
                device_id=(mates[0],), device_id_type=MESH).start()
            return

        def one(i, carry):
            pltpu.make_async_remote_copy(
                src_ref=acc.at[part, place(step, i, 1 - bits[step])], dst_ref=got[step].at[part, i],
                send_sem=send_sem.at[step, part], recv_sem=recv_sem.at[step, part],
                device_id=(mates[step],), device_id_type=MESH).start()
            return carry
        lax.fori_loop(0, got[step].shape[1], one, 0)

    def whole(step, part):
        return pltpu.make_async_remote_copy(
            src_ref=got[step].at[part], dst_ref=got[step].at[part],
            send_sem=send_sem.at[step, part], recv_sem=recv_sem.at[step, part],
            device_id=(mates[step],), device_id_type=MESH)

    def add(step, part):
        def one(i, carry):
            at = i if step == 0 else place(step, i, bits[step])
            acc[part, at] = acc[part, at] + got[step][part, i]
            return carry
        lax.fori_loop(0, got[step].shape[1], one, 0)

    def store(part):
        return pltpu.make_async_copy(acc.at[part, me // 2], out_ref.at[piece(part)], store_sem.at[part])

    for tick in range(PARTS + steps):
        for step in range(steps - 1, -1, -1):
            part = tick - 1 - step
            if 0 <= part < PARTS:
                if step == 0:
                    load(part).wait()
                whole(step, part).wait_recv()
                add(step, part)
                if step < steps - 1:
                    send(step + 1, part)
                else:
                    store(part).start()
        if tick < PARTS:
            send(0, tick)
    for part in range(PARTS):
        for step in range(steps):
            whole(step, part).wait_send()
        store(part).wait()


def reduce_scatter(x, n, cid):
    per, rest = x.shape[0] // n, x.shape[1:]
    if len(rest) == 2 or per // PARTS >= 8:
        tile, piece = (per // PARTS, None), (per // PARTS,) + rest
    else:
        tile, piece = (None, rest[0] // PARTS), (per, rest[0] // PARTS)
    steps = n.bit_length() - 1
    got = [pltpu.VMEM((PARTS, n >> (s + 1)) + piece, x.dtype) for s in range(steps)]
    size = x.size * x.dtype.itemsize
    return pl.pallas_call(
        functools.partial(reduce_kernel, tile, steps),
        out_shape=jax.ShapeDtypeStruct((per,) + rest, x.dtype),
        in_specs=[pl.BlockSpec(memory_space=pl.ANY)],
        out_specs=pl.BlockSpec(memory_space=pl.ANY),
        scratch_shapes=[pltpu.VMEM((PARTS, n // 2) + piece, x.dtype)] + got + [
            pltpu.SemaphoreType.DMA((PARTS,)),
            pltpu.SemaphoreType.DMA((steps, PARTS)),
            pltpu.SemaphoreType.DMA((steps, PARTS)),
            pltpu.SemaphoreType.DMA((PARTS,)),
        ],
        compiler_params=pltpu.CompilerParams(collective_id=cid, has_side_effects=True,
                                             vmem_limit_bytes=min(size * 3 // 2 + 4 * 2**20, 67043328)),
        name=f'reduce_{cid}',
    )(x.reshape((n // 2, 2, per) + rest))


SLOT_BITS = 1024
OUT_ROWS = 256


def pick_kernel(n, count, rows_dev, keys, first, last, table, rows_out, buf, sems):
    base = lax.axis_index('dp') * rows_dev

    def zero(i, carry):
        for slot in range(2):
            buf[slot, pl.ds(i * 32, 32)] = jnp.zeros((32,) + buf.shape[2:], buf.dtype)
        return carry

    lax.fori_loop(0, count // 32, zero, 0)

    def out_copy(j, slot):
        return pltpu.make_async_copy(buf.at[slot], rows_out.at[j], sems.at[slot])

    def per_dev(j, carry):
        slot = lax.rem(j, 2)

        @pl.when(j >= 2)
        def _():
            out_copy(j - 2, slot).wait()

            def clear(i, c):
                buf[slot, i] = jnp.zeros(buf.shape[2:], buf.dtype)
                return c

            lax.fori_loop(first[j - 2], last[j - 2], clear, 0)

        def one(i, c):
            buf[slot, i] = table[keys[j * count + i] // SLOT_BITS - base]
            return c

        lax.fori_loop(first[j], last[j], one, 0)
        out_copy(j, slot).start()
        return carry

    lax.fori_loop(0, n, per_dev, 0)
    out_copy(n - 2, 0).wait()
    out_copy(n - 1, 1).wait()


def pick_rows(table3, keys, first, last, n, count):
    smem = pl.BlockSpec(memory_space=pltpu.SMEM)
    return pl.pallas_call(
        functools.partial(pick_kernel, n, count, table3.shape[0]),
        out_shape=jax.ShapeDtypeStruct((n, count) + table3.shape[1:], table3.dtype),
        in_specs=[smem, smem, smem, pl.BlockSpec(memory_space=pltpu.VMEM)],
        out_specs=pl.BlockSpec(memory_space=pl.ANY),
        scratch_shapes=[pltpu.VMEM((2, count) + table3.shape[1:], table3.dtype), pltpu.SemaphoreType.DMA((2,))],
        compiler_params=pltpu.CompilerParams(vmem_limit_bytes=24 * 2**20),
        name='pick_rows',
    )(keys, first, last, table3)


def table_kernel(n, count, tok_dev, rows_dev, lane, keys, first, last, scale, query, cand, out_ref, acc):
    step = pl.program_id(0)
    base = lax.axis_index('dp') * rows_dev

    @pl.when(step == 0)
    def _():
        def zero(i, carry):
            acc[pl.ds(i * 64, 64)] = jnp.zeros((64,) + acc.shape[1:], jnp.float32)
            return carry

        lax.fori_loop(0, rows_dev // 64, zero, 0)

    @pl.when(step < n)
    def _():
        def one(i, carry):
            key = keys[step * count + i]
            at = key // SLOT_BITS - base
            slot = lax.rem(key, SLOT_BITS)

            @pl.when(slot < tok_dev)
            def _():
                acc[at] = acc[at] + scale[step * tok_dev + slot] * query[slot].astype(jnp.float32)

            @pl.when(slot >= tok_dev)
            def _():
                acc[at] = acc[at] + cand[slot - tok_dev]

            return carry

        lax.fori_loop(first[step], last[step], one, 0)

    @pl.when(step >= n)
    def _():
        for j in range(acc.shape[1]):
            out_ref[:, j * lane:(j + 1) * lane] = acc[pl.ds((step - n) * OUT_ROWS, OUT_ROWS), j, :]


def table_grad(keys, first, last, scale, query, cand, rows_dev, n, count):
    tok_dev, cand_dev = query.shape[0] // n, cand.shape[0] // n
    sub, lane = query.shape[1:]
    smem = pl.BlockSpec(memory_space=pltpu.SMEM)
    size = 4 * rows_dev * sub * lane
    return pl.pallas_call(
        functools.partial(table_kernel, n, count, tok_dev, rows_dev, lane),
        grid=(n + rows_dev // OUT_ROWS,),
        out_shape=jax.ShapeDtypeStruct((rows_dev, sub * lane), jnp.float32),
        in_specs=[smem, smem, smem, smem,
                  pl.BlockSpec((tok_dev, sub, lane), lambda i: (jnp.minimum(i, n - 1), 0, 0)),
                  pl.BlockSpec((cand_dev, sub, lane), lambda i: (jnp.minimum(i, n - 1), 0, 0))],
        out_specs=pl.BlockSpec((OUT_ROWS, sub * lane), lambda i: (jnp.maximum(i - n, 0), 0)),
        scratch_shapes=[pltpu.VMEM((rows_dev, sub, lane), jnp.float32)],
        cost_estimate=pl.CostEstimate(flops=30_000_000_000, bytes_accessed=4 * size, transcendentals=0),
        compiler_params=pltpu.CompilerParams(vmem_limit_bytes=size + 12 * 2**20),
        name='table_grad',
    )(keys, first, last, scale, query, cand)


def outer_kernel(left, right, out_ref):
    out_ref[...] = jnp.dot(left[...], right[...], preferred_element_type=jnp.float32)


def outer(left, right):
    rows, depth = left.shape
    cols = right.shape[1]
    high, wide = rows // 2, cols // 8
    return pl.pallas_call(
        outer_kernel,
        grid=(rows // high, cols // wide),
        out_shape=jax.ShapeDtypeStruct((rows, cols), jnp.float32),
        in_specs=[pl.BlockSpec((high, depth), lambda i, j: (i, 0)), pl.BlockSpec((depth, wide), lambda i, j: (0, j))],
        out_specs=pl.BlockSpec((high, wide), lambda i, j: (i, j)),
        cost_estimate=pl.CostEstimate(flops=2 * rows * cols * depth, bytes_accessed=4 * rows * cols, transcendentals=0),
        compiler_params=pltpu.CompilerParams(vmem_limit_bytes=16 * 2**20),
        name='outer',
    )(left, right)


def solution(mesh):
    n = mesh.shape['dp']

    def local_step(x_blk, w_one, w_two, table_blk, cand_ids, cand_logq, y_blk):
        tok_dev = x_blk.shape[0]
        rows_dev, emb_dim = table_blk.shape
        total_tok = tok_dev * n
        cand_dev = cand_ids.shape[0] // n
        count = tok_dev + cand_dev
        lane = 128
        sub = emb_dim // lane
        me = lax.axis_index('dp')

        slots = jnp.arange(count, dtype=jnp.int32)
        wants = jnp.concatenate([y_blk, lax.dynamic_slice(cand_ids, (me * cand_dev,), (cand_dev,))]) * SLOT_BITS + slots
        rank = jnp.sum((wants[None, :] < wants[:, None]).astype(jnp.int32), axis=1)
        sorted_own = jnp.sum(jnp.where(rank[:, None] == slots[None, :], wants[:, None], 0), axis=0)
        block = jnp.pad(sorted_own, (0, (-count) % (8 * lane))).reshape(-1, lane)
        everyone = spread(block, n, 0).reshape(n, -1)[:, :count]
        first = jnp.sum((everyone < me * rows_dev * SLOT_BITS).astype(jnp.int32), axis=1)
        last = jnp.sum((everyone - me * rows_dev * SLOT_BITS < rows_dev * SLOT_BITS).astype(jnp.int32), axis=1)
        keys = everyone.reshape(-1)

        picked = pick_rows(table_blk.reshape(rows_dev, sub, lane), keys, first, last, n, count)
        got = reduce_scatter(picked.reshape(n * count, sub, lane), n, 5).reshape(count, emb_dim)
        own_cand = got.at[rank[tok_dev:]].get(mode='promise_in_bounds')
        cand_rows = lax.all_gather(own_cand, 'dp', tiled=True)
        tgt_rows = got.at[rank[:tok_dev]].get(mode='promise_in_bounds')

        x_flip = lax.optimization_barrier(x_blk.T)
        pre_act = jnp.dot(x_blk, w_one, preferred_element_type=jnp.float32).astype(jnp.bfloat16)
        act_val, gelu_back = jax.vjp(jax.nn.gelu, pre_act.astype(jnp.float32))
        hidden_act = act_val.astype(jnp.bfloat16)
        query_vec = jnp.dot(hidden_act, w_two, preferred_element_type=jnp.float32).astype(jnp.bfloat16)

        z_tgt = jnp.einsum('td,td->t', query_vec, tgt_rows, preferred_element_type=jnp.float32)
        z_cand = jnp.einsum('td,sd->ts', query_vec, cand_rows, preferred_element_type=jnp.float32) - cand_logq[None, :]
        z_cand = jnp.where(y_blk[:, None] == cand_ids[None, :], -1e9, z_cand)
        peak_val = jnp.maximum(jnp.max(z_cand, axis=1), z_tgt)
        exp_total = jnp.exp(z_tgt - peak_val) + jnp.sum(jnp.exp(z_cand - peak_val[:, None]), axis=1)
        log_norm = peak_val + jnp.log(exp_total)
        loss_part = jnp.sum(log_norm - z_tgt)
        dz_tgt = (jnp.exp(z_tgt - log_norm) - 1.0) / total_tok
        dz_cand = (jnp.exp(z_cand - log_norm[:, None]) / total_tok).astype(jnp.bfloat16)
        d_query = (dz_tgt[:, None] * tgt_rows.astype(jnp.float32)
                   + jnp.dot(dz_cand, cand_rows, preferred_element_type=jnp.float32)).astype(jnp.bfloat16)

        note = jnp.concatenate([dz_tgt, jnp.broadcast_to(loss_part, (8 * lane - tok_dev,))]).reshape(8, lane)
        notes = spread(note, n, 4).reshape(n, 8 * lane)
        loss_val = jnp.sum(notes[:, tok_dev]) / total_tok
        query_all = lax.all_gather(query_vec.reshape(tok_dev, sub, lane), 'dp', tiled=True)

        part_cand = jnp.einsum('ts,td->sd', dz_cand, query_vec, preferred_element_type=jnp.float32)
        own_cand_grad = reduce_scatter(part_cand, n, 1)
        sent_cand, query_all = lax.optimization_barrier((own_cand_grad.reshape(cand_dev, sub, lane), query_all))
        cand_grad = lax.all_gather(sent_cand, 'dp', tiled=True)

        part_two = jnp.einsum('tf,td->fd', hidden_act, d_query, preferred_element_type=jnp.float32)
        part_two, own_cand_grad = lax.optimization_barrier((part_two, own_cand_grad))
        own_two = reduce_scatter(part_two, n, 2)
        sent_two, query_all = lax.optimization_barrier((own_two, query_all))
        grad_two = lax.all_gather(sent_two, 'dp', tiled=True)

        d_act = jnp.einsum('td,fd->tf', d_query, w_two, preferred_element_type=jnp.float32)
        d_pre = gelu_back(d_act.astype(jnp.bfloat16).astype(jnp.float32))[0].astype(jnp.bfloat16)
        part_one = outer(x_flip, d_pre)
        part_one, own_two = lax.optimization_barrier((part_one, own_two))
        own_one = reduce_scatter(part_one, n, 3)
        sent_one, cand_grad = lax.optimization_barrier((own_one, cand_grad))
        grad_one = lax.all_gather(sent_one, 'dp', tiled=True)

        grad_table = table_grad(keys, first, last, notes[:, :tok_dev].reshape(-1), query_all, cand_grad, rows_dev, n, count)
        return loss_val, grad_table, grad_one, grad_two

    return jax.shard_map(local_step, mesh=mesh,
                         in_specs=(P('dp', None), P(), P(), P('dp', None), P(), P(), P('dp')),
                         out_specs=(P(), P('dp', None), P(), P()), check_vma=False)
```

```python
import functools

import jax
import jax.numpy as jnp
from jax import lax
from jax.experimental import pallas as pl
from jax.experimental.pallas import tpu as pltpu
from jax.sharding import PartitionSpec as P

MESH = pl.DeviceIdType.MESH
PARTS = 8


def spread_kernel(n, in_ref, out_ref, send_sem, recv_sem):
    me = lax.axis_index('dp')
    barrier = pltpu.get_barrier_semaphore()

    def greet(i, carry):
        pl.semaphore_signal(barrier, inc=1, device_id=(lax.rem(me + i, n),), device_id_type=MESH)
        return carry

    lax.fori_loop(1, n, greet, 0)
    pl.semaphore_wait(barrier, n - 1)

    def send(i, carry):
        pltpu.make_async_remote_copy(
            src_ref=in_ref, dst_ref=out_ref.at[me], send_sem=send_sem, recv_sem=recv_sem,
            device_id=(lax.rem(me + i, n),), device_id_type=MESH).start()
        return carry

    lax.fori_loop(1, n, send, 0)
    others = out_ref.at[pl.ds(0, n - 1)]
    drain = pltpu.make_async_remote_copy(
        src_ref=others, dst_ref=others, send_sem=send_sem, recv_sem=recv_sem,
        device_id=(me,), device_id_type=MESH)
    drain.wait_recv()
    drain.wait_send()
    out_ref[me] = in_ref[...]


def spread(block, n, cid):
    return pl.pallas_call(
        functools.partial(spread_kernel, n),
        out_shape=jax.ShapeDtypeStruct((n,) + block.shape, block.dtype),
        in_specs=[pl.BlockSpec(memory_space=pltpu.VMEM)],
        out_specs=pl.BlockSpec(memory_space=pltpu.VMEM),
        scratch_shapes=[pltpu.SemaphoreType.DMA, pltpu.SemaphoreType.DMA],
        compiler_params=pltpu.CompilerParams(collective_id=cid, has_side_effects=True),
        name=f'spread_{cid}',
    )(block)


def reduce_kernel(tile, steps, in_ref, out_ref, acc, *scratch):
    got, (load_sem, send_sem, recv_sem, store_sem) = scratch[:steps], scratch[steps:]
    me = lax.axis_index('dp')
    core = lax.rem(me, 2)
    xb, yb = lax.rem(me // 2, 2), lax.rem(me // 4, 2)
    z0, z1 = lax.rem(me // 8, 2), lax.rem(me // 16, 2)
    one = (1 + core, xb * (1 - core) + yb * core)
    two = (2 - core, yb * (1 - core) + xb * core)
    ways = ((one, two, (4, z0), (8, z1))[:steps - 1], ((4, z0), (8, z1), one, two)[-steps + 1:] if steps > 4 else ((4, z0), one, two))

    def way(part):
        return ways[1 if part % 4 == 1 else 0]

    def mate(step, part):
        if step == 0:
            return me + 1 - 2 * core
        weight, bit = way(part)[step - 1]
        return me + 2 * weight * (1 - 2 * bit)

    mates = [mate(step, 0) for step in range(steps)]
    barrier = pltpu.get_barrier_semaphore()
    for other in mates:
        pl.semaphore_signal(barrier, inc=1, device_id=(other,), device_id_type=MESH)

    def piece(part):
        if tile[0] is None:
            return (slice(None), pl.ds(part * tile[1], tile[1]))
        return (pl.ds(part * tile[0], tile[0]),)

    def load(part):
        return pltpu.make_async_copy(in_ref.at[(slice(None), core) + piece(part)], acc.at[part], load_sem.at[part])

    for part in range(PARTS):
        load(part).start()
    pl.semaphore_wait(barrier, steps)

    def place(step, part, i, theirs):
        dims = way(part)
        weight, bit = dims[step - 1]
        at = weight * (1 - bit if theirs else bit)
        for w, own in dims[:step - 1]:
            at = at + w * own
        for k, (w, _) in enumerate(dims[step:]):
            at = at + w * lax.rem(i // 2 ** k, 2)
        return at

    def send(step, part):
        if step == 0:
            pltpu.make_async_remote_copy(
                src_ref=in_ref.at[(slice(None), 1 - core) + piece(part)], dst_ref=got[0].at[part],
                send_sem=send_sem.at[0, part], recv_sem=recv_sem.at[0, part],
                device_id=(mate(0, part),), device_id_type=MESH).start()
            return

        def one(i, carry):
            pltpu.make_async_remote_copy(
                src_ref=acc.at[part, place(step, part, i, True)], dst_ref=got[step].at[part, i],
                send_sem=send_sem.at[step, part], recv_sem=recv_sem.at[step, part],
                device_id=(mate(step, part),), device_id_type=MESH).start()
            return carry
        lax.fori_loop(0, got[step].shape[1], one, 0)

    def whole(step, part):
        return pltpu.make_async_remote_copy(
            src_ref=got[step].at[part], dst_ref=got[step].at[part],
            send_sem=send_sem.at[step, part], recv_sem=recv_sem.at[step, part],
            device_id=(mate(step, part),), device_id_type=MESH)

    def add(step, part):
        def one(i, carry):
            at = i if step == 0 else place(step, part, i, False)
            acc[part, at] = acc[part, at] + got[step][part, i]
            return carry
        lax.fori_loop(0, got[step].shape[1], one, 0)

    def store(part):
        return pltpu.make_async_copy(acc.at[part, me // 2], out_ref.at[piece(part)], store_sem.at[part])

    for tick in range(PARTS + steps):
        if tick < PARTS:
            send(0, tick)
        for step in range(steps):
            part = tick - 1 - step
            if 0 <= part < PARTS:
                if step == 0:
                    load(part).wait()
                whole(step, part).wait_recv()
                add(step, part)
                if step < steps - 1:
                    send(step + 1, part)
                else:
                    store(part).start()
    for part in range(PARTS):
        for step in range(steps):
            whole(step, part).wait_send()
        store(part).wait()


def reduce_scatter(x, n, cid):
    per, rest = x.shape[0] // n, x.shape[1:]
    if len(rest) == 2 or per // PARTS >= 8:
        tile, piece = (per // PARTS, None), (per // PARTS,) + rest
    else:
        tile, piece = (None, rest[0] // PARTS), (per, rest[0] // PARTS)
    steps = n.bit_length() - 1
    got = [pltpu.VMEM((PARTS, n >> (s + 1)) + piece, x.dtype) for s in range(steps)]
    size = x.size * x.dtype.itemsize
    return pl.pallas_call(
        functools.partial(reduce_kernel, tile, steps),
        out_shape=jax.ShapeDtypeStruct((per,) + rest, x.dtype),
        in_specs=[pl.BlockSpec(memory_space=pl.ANY)],
        out_specs=pl.BlockSpec(memory_space=pl.ANY),
        scratch_shapes=[pltpu.VMEM((PARTS, n // 2) + piece, x.dtype)] + got + [
            pltpu.SemaphoreType.DMA((PARTS,)),
            pltpu.SemaphoreType.DMA((steps, PARTS)),
            pltpu.SemaphoreType.DMA((steps, PARTS)),
            pltpu.SemaphoreType.DMA((PARTS,)),
        ],
        compiler_params=pltpu.CompilerParams(collective_id=cid, has_side_effects=True,
                                             vmem_limit_bytes=min(size * 3 // 2 + 4 * 2**20, 67043328)),
        name=f'reduce_{cid}',
    )(x.reshape((n // 2, 2, per) + rest))


SLOT_BITS = 1024
OUT_ROWS = 256


def pick_kernel(n, count, rows_dev, keys, first, last, table, tgt_out, cand_out, buf, sems):
    base = lax.axis_index('dp') * rows_dev
    tok_dev = tgt_out.shape[1]

    def zero(i, carry):
        for side in range(2):
            buf[side, pl.ds(i * 32, 32)] = jnp.zeros((32,) + buf.shape[2:], buf.dtype)
        return carry

    lax.fori_loop(0, count // 32, zero, 0)

    def out_copies(j, side):
        return (pltpu.make_async_copy(buf.at[side, pl.ds(0, tok_dev)], tgt_out.at[j], sems.at[side, 0]),
                pltpu.make_async_copy(buf.at[side, pl.ds(tok_dev, count - tok_dev)], cand_out.at[j], sems.at[side, 1]))

    def per_dev(j, carry):
        side = lax.rem(j, 2)

        @pl.when(j >= 2)
        def _():
            for copy in out_copies(j - 2, side):
                copy.wait()

            def clear(i, c):
                buf[side, lax.rem(keys[(j - 2) * count + i], SLOT_BITS)] = jnp.zeros(buf.shape[2:], buf.dtype)
                return c

            lax.fori_loop(first[j - 2], last[j - 2], clear, 0)

        def one(i, c):
            key = keys[j * count + i]
            buf[side, lax.rem(key, SLOT_BITS)] = table[key // SLOT_BITS - base]
            return c

        lax.fori_loop(first[j], last[j], one, 0)
        for copy in out_copies(j, side):
            copy.start()
        return carry

    lax.fori_loop(0, n, per_dev, 0)
    for copy in out_copies(n - 2, 0) + out_copies(n - 1, 1):
        copy.wait()


def pick_rows(table3, keys, first, last, n, count, tok_dev):
    smem = pl.BlockSpec(memory_space=pltpu.SMEM)
    anywhere = pl.BlockSpec(memory_space=pl.ANY)
    tail = table3.shape[1:]
    return pl.pallas_call(
        functools.partial(pick_kernel, n, count, table3.shape[0]),
        out_shape=(jax.ShapeDtypeStruct((n, tok_dev) + tail, table3.dtype),
                   jax.ShapeDtypeStruct((n, count - tok_dev) + tail, table3.dtype)),
        in_specs=[smem, smem, smem, pl.BlockSpec(memory_space=pltpu.VMEM)],
        out_specs=(anywhere, anywhere),
        scratch_shapes=[pltpu.VMEM((2, count) + tail, table3.dtype), pltpu.SemaphoreType.DMA((2, 2))],
        compiler_params=pltpu.CompilerParams(vmem_limit_bytes=24 * 2**20),
        name='pick_rows',
    )(keys, first, last, table3)


def table_kernel(n, count, tok_dev, rows_dev, lane, keys, first, last, scale, query, cand, out_ref, acc):
    step = pl.program_id(0)
    base = lax.axis_index('dp') * rows_dev

    @pl.when(step == 0)
    def _():
        def zero(i, carry):
            acc[pl.ds(i * 64, 64)] = jnp.zeros((64,) + acc.shape[1:], jnp.float32)
            return carry

        lax.fori_loop(0, rows_dev // 64, zero, 0)

    @pl.when(step < n)
    def _():
        def one(i, carry):
            key = keys[step * count + i]
            at = key // SLOT_BITS - base
            slot = lax.rem(key, SLOT_BITS)

            @pl.when(slot < tok_dev)
            def _():
                acc[at] = acc[at] + scale[step * tok_dev + slot] * query[slot].astype(jnp.float32)

            @pl.when(slot >= tok_dev)
            def _():
                acc[at] = acc[at] + cand[slot - tok_dev]

            return carry

        lax.fori_loop(first[step], last[step], one, 0)

    @pl.when(step >= n)
    def _():
        for j in range(acc.shape[1]):
            out_ref[:, j * lane:(j + 1) * lane] = acc[pl.ds((step - n) * OUT_ROWS, OUT_ROWS), j, :]


def table_grad(keys, first, last, scale, query, cand, rows_dev, n, count):
    tok_dev, cand_dev = query.shape[0] // n, cand.shape[0] // n
    sub, lane = query.shape[1:]
    smem = pl.BlockSpec(memory_space=pltpu.SMEM)
    size = 4 * rows_dev * sub * lane
    return pl.pallas_call(
        functools.partial(table_kernel, n, count, tok_dev, rows_dev, lane),
        grid=(n + rows_dev // OUT_ROWS,),
        out_shape=jax.ShapeDtypeStruct((rows_dev, sub * lane), jnp.float32),
        in_specs=[smem, smem, smem, smem,
                  pl.BlockSpec((tok_dev, sub, lane), lambda i: (jnp.minimum(i, n - 1), 0, 0)),
                  pl.BlockSpec((cand_dev, sub, lane), lambda i: (jnp.minimum(i, n - 1), 0, 0))],
        out_specs=pl.BlockSpec((OUT_ROWS, sub * lane), lambda i: (jnp.maximum(i - n, 0), 0)),
        scratch_shapes=[pltpu.VMEM((rows_dev, sub, lane), jnp.float32)],
        cost_estimate=pl.CostEstimate(flops=30_000_000_000, bytes_accessed=4 * size, transcendentals=0),
        compiler_params=pltpu.CompilerParams(vmem_limit_bytes=size + 12 * 2**20),
        name='table_grad',
    )(keys, first, last, scale, query, cand)


def outer_kernel(left, right, out_ref):
    out_ref[...] = jnp.dot(left[...], right[...], preferred_element_type=jnp.float32)


def outer(left, right):
    rows, depth = left.shape
    cols = right.shape[1]
    high, wide = rows // 2, cols // 8
    return pl.pallas_call(
        outer_kernel,
        grid=(rows // high, cols // wide),
        out_shape=jax.ShapeDtypeStruct((rows, cols), jnp.float32),
        in_specs=[pl.BlockSpec((high, depth), lambda i, j: (i, 0)), pl.BlockSpec((depth, wide), lambda i, j: (0, j))],
        out_specs=pl.BlockSpec((high, wide), lambda i, j: (i, j)),
        cost_estimate=pl.CostEstimate(flops=2 * rows * cols * depth, bytes_accessed=4 * rows * cols, transcendentals=0),
        compiler_params=pltpu.CompilerParams(vmem_limit_bytes=16 * 2**20),
        name='outer',
    )(left, right)


def solution(mesh):
    n = mesh.shape['dp']

    def local_step(x_blk, w_one, w_two, table_blk, cand_ids, cand_logq, y_blk):
        tok_dev = x_blk.shape[0]
        rows_dev, emb_dim = table_blk.shape
        total_tok = tok_dev * n
        cand_dev = cand_ids.shape[0] // n
        count = tok_dev + cand_dev
        lane = 128
        sub = emb_dim // lane
        me = lax.axis_index('dp')

        slots = jnp.arange(count, dtype=jnp.int32)
        wants = jnp.concatenate([y_blk, lax.dynamic_slice(cand_ids, (me * cand_dev,), (cand_dev,))]) * SLOT_BITS + slots
        rank = jnp.sum((wants[None, :] < wants[:, None]).astype(jnp.int32), axis=1)
        sorted_own = jnp.sum(jnp.where(rank[:, None] == slots[None, :], wants[:, None], 0), axis=0)
        block = jnp.pad(sorted_own, (0, (-count) % (8 * lane))).reshape(-1, lane)
        everyone = spread(block, n, 0).reshape(n, -1)[:, :count]
        first = jnp.sum((everyone < me * rows_dev * SLOT_BITS).astype(jnp.int32), axis=1)
        last = jnp.sum((everyone - me * rows_dev * SLOT_BITS < rows_dev * SLOT_BITS).astype(jnp.int32), axis=1)
        keys = everyone.reshape(-1)

        tgt_part, cand_part = pick_rows(table_blk.reshape(rows_dev, sub, lane), keys, first, last, n, count, tok_dev)
        own_cand = reduce_scatter(cand_part.reshape(n * cand_dev, sub, lane), n, 5).reshape(cand_dev, emb_dim)
        cand_rows = lax.all_gather(own_cand, 'dp', tiled=True)

        x_flip = lax.optimization_barrier(x_blk.T)
        pre_act = jnp.dot(x_blk, w_one, preferred_element_type=jnp.float32).astype(jnp.bfloat16)
        act_val, gelu_back = jax.vjp(jax.nn.gelu, pre_act.astype(jnp.float32))
        hidden_act = act_val.astype(jnp.bfloat16)
        query_vec = jnp.dot(hidden_act, w_two, preferred_element_type=jnp.float32).astype(jnp.bfloat16)
        query_all = lax.all_gather(query_vec.reshape(tok_dev, sub, lane), 'dp', tiled=True)
        tgt_part, query_vec = lax.optimization_barrier((tgt_part, query_vec))
        tgt_rows = reduce_scatter(tgt_part.reshape(n * tok_dev, sub, lane), n, 6).reshape(tok_dev, emb_dim)

        z_tgt = jnp.einsum('td,td->t', query_vec, tgt_rows, preferred_element_type=jnp.float32)
        z_cand = jnp.einsum('td,sd->ts', query_vec, cand_rows, preferred_element_type=jnp.float32) - cand_logq[None, :]
        z_cand = jnp.where(y_blk[:, None] == cand_ids[None, :], -1e9, z_cand)
        peak_val = jnp.maximum(jnp.max(z_cand, axis=1), z_tgt)
        exp_total = jnp.exp(z_tgt - peak_val) + jnp.sum(jnp.exp(z_cand - peak_val[:, None]), axis=1)
        log_norm = peak_val + jnp.log(exp_total)
        loss_part = jnp.sum(log_norm - z_tgt)
        dz_tgt = (jnp.exp(z_tgt - log_norm) - 1.0) / total_tok
        dz_cand = (jnp.exp(z_cand - log_norm[:, None]) / total_tok).astype(jnp.bfloat16)
        d_query = (dz_tgt[:, None] * tgt_rows.astype(jnp.float32)
                   + jnp.dot(dz_cand, cand_rows, preferred_element_type=jnp.float32)).astype(jnp.bfloat16)

        note = jnp.concatenate([dz_tgt, jnp.broadcast_to(loss_part, (8 * lane - tok_dev,))]).reshape(8, lane)
        notes = spread(note, n, 4).reshape(n, 8 * lane)
        loss_val = jnp.sum(notes[:, tok_dev]) / total_tok
        part_cand = jnp.einsum('ts,td->sd', dz_cand, query_vec, preferred_element_type=jnp.float32)
        own_cand_grad = reduce_scatter(part_cand, n, 1)
        sent_cand, query_all = lax.optimization_barrier((own_cand_grad.reshape(cand_dev, sub, lane), query_all))
        cand_grad = lax.all_gather(sent_cand, 'dp', tiled=True)

        part_two = jnp.einsum('tf,td->fd', hidden_act, d_query, preferred_element_type=jnp.float32)
        part_two, own_cand_grad = lax.optimization_barrier((part_two, own_cand_grad))
        own_two = reduce_scatter(part_two, n, 2)
        sent_two, query_all = lax.optimization_barrier((own_two, query_all))
        grad_two = lax.all_gather(sent_two, 'dp', tiled=True)

        d_act = jnp.einsum('td,fd->tf', d_query, w_two, preferred_element_type=jnp.float32)
        d_pre = gelu_back(d_act.astype(jnp.bfloat16).astype(jnp.float32))[0].astype(jnp.bfloat16)
        part_one = outer(x_flip, d_pre)
        part_one, own_two = lax.optimization_barrier((part_one, own_two))
        own_one = reduce_scatter(part_one, n, 3)
        sent_one, cand_grad = lax.optimization_barrier((own_one, cand_grad))
        grad_one = lax.all_gather(sent_one, 'dp', tiled=True)

        grad_table = table_grad(keys, first, last, notes[:, :tok_dev].reshape(-1), query_all, cand_grad, rows_dev, n, count)
        return loss_val, grad_table, grad_one, grad_two

    return jax.shard_map(local_step, mesh=mesh,
                         in_specs=(P('dp', None), P(), P(), P('dp', None), P(), P(), P('dp')),
                         out_specs=(P(), P('dp', None), P(), P()), check_vma=False)
```

```python
import functools

import jax
import jax.numpy as jnp
from jax import lax
from jax.experimental import pallas as pl
from jax.experimental.pallas import tpu as pltpu
from jax.sharding import PartitionSpec as P

MESH = pl.DeviceIdType.MESH
PARTS = 16


def spread_kernel(n, in_ref, out_ref, send_sem, recv_sem):
    me = lax.axis_index('dp')
    barrier = pltpu.get_barrier_semaphore()

    def greet(i, carry):
        pl.semaphore_signal(barrier, inc=1, device_id=(lax.rem(me + i, n),), device_id_type=MESH)
        return carry

    lax.fori_loop(1, n, greet, 0)
    pl.semaphore_wait(barrier, n - 1)

    def send(i, carry):
        pltpu.make_async_remote_copy(
            src_ref=in_ref, dst_ref=out_ref.at[me], send_sem=send_sem, recv_sem=recv_sem,
            device_id=(lax.rem(me + i, n),), device_id_type=MESH).start()
        return carry

    lax.fori_loop(1, n, send, 0)
    others = out_ref.at[pl.ds(0, n - 1)]
    drain = pltpu.make_async_remote_copy(
        src_ref=others, dst_ref=others, send_sem=send_sem, recv_sem=recv_sem,
        device_id=(me,), device_id_type=MESH)
    drain.wait_recv()
    drain.wait_send()
    out_ref[me] = in_ref[...]


def spread(block, n, cid):
    return pl.pallas_call(
        functools.partial(spread_kernel, n),
        out_shape=jax.ShapeDtypeStruct((n,) + block.shape, block.dtype),
        in_specs=[pl.BlockSpec(memory_space=pltpu.VMEM)],
        out_specs=pl.BlockSpec(memory_space=pltpu.VMEM),
        scratch_shapes=[pltpu.SemaphoreType.DMA, pltpu.SemaphoreType.DMA],
        compiler_params=pltpu.CompilerParams(collective_id=cid, has_side_effects=True),
        name=f'spread_{cid}',
    )(block)


def reduce_kernel(tile, steps, in_ref, out_ref, acc, *scratch):
    got, (load_sem, send_sem, recv_sem, store_sem) = scratch[:steps], scratch[steps:]
    me = lax.axis_index('dp')
    core = lax.rem(me, 2)
    xb, yb = lax.rem(me // 2, 2), lax.rem(me // 4, 2)
    z0, z1 = lax.rem(me // 8, 2), lax.rem(me // 16, 2)
    one = (1 + core, xb * (1 - core) + yb * core)
    two = (2 - core, yb * (1 - core) + xb * core)
    plain = (one, two, (4, z0), (8, z1))[:steps - 1]
    turned = ((4, z0), (8, z1), one, two) if steps > 4 else ((4, z0), one, two)

    def way(part):
        flip = 1 if isinstance(part, int) and part % 4 == 1 else 0
        if not isinstance(part, int):
            flip = (lax.rem(part, 4) + 3) // 4 * (1 - lax.rem(part, 4) // 2)
        return [(p + flip * (t - p), q + flip * (u - q)) for (p, q), (t, u) in zip(plain, turned)]

    def mate(step, part):
        if step == 0:
            return me + 1 - 2 * core
        weight, bit = way(part)[step - 1]
        return me + 2 * weight * (1 - 2 * bit)

    mates = [mate(step, 0) for step in range(steps)]
    barrier = pltpu.get_barrier_semaphore()
    for other in mates:
        pl.semaphore_signal(barrier, inc=1, device_id=(other,), device_id_type=MESH)

    def piece(part):
        if tile[0] is None:
            return (slice(None), pl.ds(pl.multiple_of(part * tile[1], tile[1]), tile[1]))
        return (pl.ds(pl.multiple_of(part * tile[0], tile[0]), tile[0]),)

    def load(part):
        return pltpu.make_async_copy(in_ref.at[(slice(None), core) + piece(part)], acc.at[part], load_sem.at[part])

    def begin(part, carry):
        load(part).start()
        return carry

    lax.fori_loop(0, PARTS, begin, 0)
    pl.semaphore_wait(barrier, steps)

    def place(step, part, i, theirs):
        dims = way(part)
        weight, bit = dims[step - 1]
        at = weight * (1 - bit if theirs else bit)
        for w, own in dims[:step - 1]:
            at = at + w * own
        for k, (w, _) in enumerate(dims[step:]):
            at = at + w * lax.rem(i // 2 ** k, 2)
        return at

    def send(step, part):
        if step == 0:
            pltpu.make_async_remote_copy(
                src_ref=in_ref.at[(slice(None), 1 - core) + piece(part)], dst_ref=got[0].at[part],
                send_sem=send_sem.at[0, part], recv_sem=recv_sem.at[0, part],
                device_id=(mate(0, part),), device_id_type=MESH).start()
            return

        def one(i, carry):
            pltpu.make_async_remote_copy(
                src_ref=acc.at[part, place(step, part, i, True)], dst_ref=got[step].at[part, i],
                send_sem=send_sem.at[step, part], recv_sem=recv_sem.at[step, part],
                device_id=(mate(step, part),), device_id_type=MESH).start()
            return carry
        lax.fori_loop(0, got[step].shape[1], one, 0)

    def whole(step, part):
        return pltpu.make_async_remote_copy(
            src_ref=got[step].at[part], dst_ref=got[step].at[part],
            send_sem=send_sem.at[step, part], recv_sem=recv_sem.at[step, part],
            device_id=(mate(step, part),), device_id_type=MESH)

    def add(step, part):
        def one(i, carry):
            at = i if step == 0 else place(step, part, i, False)
            acc[part, at] = acc[part, at] + got[step][part, i]
            return carry
        lax.fori_loop(0, got[step].shape[1], one, 0)

    def store(part):
        return pltpu.make_async_copy(acc.at[part, me // 2], out_ref.at[piece(part)], store_sem.at[part])

    def tick(t, carry):
        @pl.when(t < PARTS)
        def _():
            send(0, t)

        for step in range(steps):
            part = t - 1 - step

            @pl.when((part >= 0) & (part < PARTS))
            def _():
                if step == 0:
                    load(part).wait()
                whole(step, part).wait_recv()
                add(step, part)
                if step < steps - 1:
                    send(step + 1, part)
                else:
                    store(part).start()

        return carry

    lax.fori_loop(0, PARTS + steps, tick, 0)

    def finish(part, carry):
        for step in range(steps):
            whole(step, part).wait_send()
        store(part).wait()
        return carry

    lax.fori_loop(0, PARTS, finish, 0)


def reduce_scatter(x, n, cid):
    per, rest = x.shape[0] // n, x.shape[1:]
    if len(rest) == 2 or per // PARTS >= 8:
        tile, piece = (per // PARTS, None), (per // PARTS,) + rest
    else:
        tile, piece = (None, rest[0] // PARTS), (per, rest[0] // PARTS)
    steps = n.bit_length() - 1
    got = [pltpu.VMEM((PARTS, n >> (s + 1)) + piece, x.dtype) for s in range(steps)]
    size = x.size * x.dtype.itemsize
    return pl.pallas_call(
        functools.partial(reduce_kernel, tile, steps),
        out_shape=jax.ShapeDtypeStruct((per,) + rest, x.dtype),
        in_specs=[pl.BlockSpec(memory_space=pl.ANY)],
        out_specs=pl.BlockSpec(memory_space=pl.ANY),
        scratch_shapes=[pltpu.VMEM((PARTS, n // 2) + piece, x.dtype)] + got + [
            pltpu.SemaphoreType.DMA((PARTS,)),
            pltpu.SemaphoreType.DMA((steps, PARTS)),
            pltpu.SemaphoreType.DMA((steps, PARTS)),
            pltpu.SemaphoreType.DMA((PARTS,)),
        ],
        compiler_params=pltpu.CompilerParams(collective_id=cid, has_side_effects=True,
                                             vmem_limit_bytes=min(size * 3 // 2 + 4 * 2**20, 67043328)),
        name=f'reduce_{cid}',
    )(x.reshape((n // 2, 2, per) + rest))


SLOT_BITS = 1024
OUT_ROWS = 256


def pick_kernel(n, count, rows_dev, keys, first, last, table, tgt_out, cand_out, buf, sems):
    base = lax.axis_index('dp') * rows_dev
    tok_dev = tgt_out.shape[1]

    def zero(i, carry):
        for side in range(2):
            buf[side, pl.ds(i * 32, 32)] = jnp.zeros((32,) + buf.shape[2:], buf.dtype)
        return carry

    lax.fori_loop(0, count // 32, zero, 0)

    def out_copies(j, side):
        return (pltpu.make_async_copy(buf.at[side, pl.ds(0, tok_dev)], tgt_out.at[j], sems.at[side, 0]),
                pltpu.make_async_copy(buf.at[side, pl.ds(tok_dev, count - tok_dev)], cand_out.at[j], sems.at[side, 1]))

    def per_dev(j, carry):
        side = lax.rem(j, 2)

        @pl.when(j >= 2)
        def _():
            for copy in out_copies(j - 2, side):
                copy.wait()

            def clear(i, c):
                buf[side, lax.rem(keys[(j - 2) * count + i], SLOT_BITS)] = jnp.zeros(buf.shape[2:], buf.dtype)
                return c

            lax.fori_loop(first[j - 2], last[j - 2], clear, 0)

        def one(i, c):
            key = keys[j * count + i]
            buf[side, lax.rem(key, SLOT_BITS)] = table[key // SLOT_BITS - base]
            return c

        lax.fori_loop(first[j], last[j], one, 0)
        for copy in out_copies(j, side):
            copy.start()
        return carry

    lax.fori_loop(0, n, per_dev, 0)
    for copy in out_copies(n - 2, 0) + out_copies(n - 1, 1):
        copy.wait()


def pick_rows(table3, keys, first, last, n, count, tok_dev):
    smem = pl.BlockSpec(memory_space=pltpu.SMEM)
    anywhere = pl.BlockSpec(memory_space=pl.ANY)
    tail = table3.shape[1:]
    return pl.pallas_call(
        functools.partial(pick_kernel, n, count, table3.shape[0]),
        out_shape=(jax.ShapeDtypeStruct((n, tok_dev) + tail, table3.dtype),
                   jax.ShapeDtypeStruct((n, count - tok_dev) + tail, table3.dtype)),
        in_specs=[smem, smem, smem, pl.BlockSpec(memory_space=pltpu.VMEM)],
        out_specs=(anywhere, anywhere),
        scratch_shapes=[pltpu.VMEM((2, count) + tail, table3.dtype), pltpu.SemaphoreType.DMA((2, 2))],
        compiler_params=pltpu.CompilerParams(vmem_limit_bytes=24 * 2**20),
        name='pick_rows',
    )(keys, first, last, table3)


def table_kernel(n, count, tok_dev, rows_dev, lane, keys, first, last, scale, query, cand, out_ref, acc):
    step = pl.program_id(0)
    base = lax.axis_index('dp') * rows_dev

    @pl.when(step == 0)
    def _():
        def zero(i, carry):
            acc[pl.ds(i * 64, 64)] = jnp.zeros((64,) + acc.shape[1:], jnp.float32)
            return carry

        lax.fori_loop(0, rows_dev // 64, zero, 0)

    @pl.when(step < n)
    def _():
        def one(i, carry):
            key = keys[step * count + i]
            at = key // SLOT_BITS - base
            slot = lax.rem(key, SLOT_BITS)

            @pl.when(slot < tok_dev)
            def _():
                acc[at] = acc[at] + scale[step * tok_dev + slot] * query[slot].astype(jnp.float32)

            @pl.when(slot >= tok_dev)
            def _():
                acc[at] = acc[at] + cand[slot - tok_dev]

            return carry

        lax.fori_loop(first[step], last[step], one, 0)

    @pl.when(step >= n)
    def _():
        for j in range(acc.shape[1]):
            out_ref[:, j * lane:(j + 1) * lane] = acc[pl.ds((step - n) * OUT_ROWS, OUT_ROWS), j, :]


def table_grad(keys, first, last, scale, query, cand, rows_dev, n, count):
    tok_dev, cand_dev = query.shape[0] // n, cand.shape[0] // n
    sub, lane = query.shape[1:]
    smem = pl.BlockSpec(memory_space=pltpu.SMEM)
    size = 4 * rows_dev * sub * lane
    return pl.pallas_call(
        functools.partial(table_kernel, n, count, tok_dev, rows_dev, lane),
        grid=(n + rows_dev // OUT_ROWS,),
        out_shape=jax.ShapeDtypeStruct((rows_dev, sub * lane), jnp.float32),
        in_specs=[smem, smem, smem, smem,
                  pl.BlockSpec((tok_dev, sub, lane), lambda i: (jnp.minimum(i, n - 1), 0, 0)),
                  pl.BlockSpec((cand_dev, sub, lane), lambda i: (jnp.minimum(i, n - 1), 0, 0))],
        out_specs=pl.BlockSpec((OUT_ROWS, sub * lane), lambda i: (jnp.maximum(i - n, 0), 0)),
        scratch_shapes=[pltpu.VMEM((rows_dev, sub, lane), jnp.float32)],
        cost_estimate=pl.CostEstimate(flops=30_000_000_000, bytes_accessed=4 * size, transcendentals=0),
        compiler_params=pltpu.CompilerParams(vmem_limit_bytes=size + 12 * 2**20),
        name='table_grad',
    )(keys, first, last, scale, query, cand)


def outer_kernel(left, right, out_ref):
    out_ref[...] = jnp.dot(left[...], right[...], preferred_element_type=jnp.float32)


def outer(left, right):
    rows, depth = left.shape
    cols = right.shape[1]
    high, wide = rows, cols // 8
    return pl.pallas_call(
        outer_kernel,
        grid=(rows // high, cols // wide),
        out_shape=jax.ShapeDtypeStruct((rows, cols), jnp.float32),
        in_specs=[pl.BlockSpec((high, depth), lambda i, j: (i, 0)), pl.BlockSpec((depth, wide), lambda i, j: (0, j))],
        out_specs=pl.BlockSpec((high, wide), lambda i, j: (i, j)),
        cost_estimate=pl.CostEstimate(flops=2 * rows * cols * depth, bytes_accessed=4 * rows * cols, transcendentals=0),
        compiler_params=pltpu.CompilerParams(vmem_limit_bytes=16 * 2**20),
        name='outer',
    )(left, right)


def carry_kernel(in_ref, out_ref):
    out_ref[...] = in_ref[...]


def carry_over(x):
    rows, cols = x.shape
    spec = pl.BlockSpec((rows // 8, cols), lambda i: (i, 0))
    return pl.pallas_call(
        carry_kernel, grid=(8,), out_shape=jax.ShapeDtypeStruct(x.shape, x.dtype), in_specs=[spec], out_specs=spec,
        cost_estimate=pl.CostEstimate(flops=x.size, bytes_accessed=8 * x.size, transcendentals=0),
        compiler_params=pltpu.CompilerParams(vmem_limit_bytes=16 * 2**20), name='carry_over')(x)


def fill_low(x):
    rows, cols = x.shape
    spec = pl.BlockSpec((rows // 4, cols), lambda i: (i, 0))
    return pl.pallas_call(
        carry_kernel, grid=(4,), out_shape=jax.ShapeDtypeStruct((2 * rows, cols), x.dtype), in_specs=[spec], out_specs=spec,
        cost_estimate=pl.CostEstimate(flops=x.size, bytes_accessed=8 * x.size, transcendentals=0),
        compiler_params=pltpu.CompilerParams(vmem_limit_bytes=16 * 2**20), name='fill_low')(x)


def high_kernel(whole_ref, in_ref, out_ref):
    out_ref[...] = in_ref[...]


def fill_high(whole, x):
    rows, cols = x.shape
    return pl.pallas_call(
        high_kernel, grid=(4,), out_shape=jax.ShapeDtypeStruct(whole.shape, x.dtype),
        in_specs=[pl.BlockSpec(memory_space=pl.ANY), pl.BlockSpec((rows // 4, cols), lambda i: (i, 0))],
        out_specs=pl.BlockSpec((rows // 4, cols), lambda i: (i + 4, 0)), input_output_aliases={0: 0},
        cost_estimate=pl.CostEstimate(flops=x.size, bytes_accessed=8 * x.size, transcendentals=0),
        compiler_params=pltpu.CompilerParams(vmem_limit_bytes=16 * 2**20), name='fill_high')(whole, x)


def solution(mesh):
    n = mesh.shape['dp']

    def local_step(x_blk, w_one, w_two, table_blk, cand_ids, cand_logq, y_blk):
        tok_dev = x_blk.shape[0]
        rows_dev, emb_dim = table_blk.shape
        total_tok = tok_dev * n
        cand_dev = cand_ids.shape[0] // n
        count = tok_dev + cand_dev
        lane = 128
        sub = emb_dim // lane
        me = lax.axis_index('dp')

        slots = jnp.arange(count, dtype=jnp.int32)
        wants = jnp.concatenate([y_blk, lax.dynamic_slice(cand_ids, (me * cand_dev,), (cand_dev,))]) * SLOT_BITS + slots
        rank = jnp.sum((wants[None, :] < wants[:, None]).astype(jnp.int32), axis=1)
        sorted_own = jnp.sum(jnp.where(rank[:, None] == slots[None, :], wants[:, None], 0), axis=0)
        block = jnp.pad(sorted_own, (0, (-count) % (8 * lane))).reshape(-1, lane)
        everyone = spread(block, n, 0).reshape(n, -1)[:, :count]
        first = jnp.sum((everyone < me * rows_dev * SLOT_BITS).astype(jnp.int32), axis=1)
        last = jnp.sum((everyone - me * rows_dev * SLOT_BITS < rows_dev * SLOT_BITS).astype(jnp.int32), axis=1)
        keys = everyone.reshape(-1)

        tgt_part, cand_part = pick_rows(table_blk.reshape(rows_dev, sub, lane), keys, first, last, n, count, tok_dev)
        own_cand = reduce_scatter(cand_part.reshape(n * cand_dev, sub, lane), n, 5).reshape(cand_dev, emb_dim)
        cand_rows = lax.all_gather(own_cand, 'dp', tiled=True)

        x_flip = lax.optimization_barrier(x_blk.T)
        pre_act = jnp.dot(x_blk, w_one, preferred_element_type=jnp.float32).astype(jnp.bfloat16)
        act_val, gelu_back = jax.vjp(jax.nn.gelu, pre_act.astype(jnp.float32))
        hidden_act = act_val.astype(jnp.bfloat16)
        query_vec = jnp.dot(hidden_act, w_two, preferred_element_type=jnp.float32).astype(jnp.bfloat16)
        query_all = lax.all_gather(query_vec.reshape(tok_dev, sub, lane), 'dp', tiled=True)
        tgt_part, query_vec = lax.optimization_barrier((tgt_part, query_vec))
        tgt_rows = reduce_scatter(tgt_part.reshape(n * tok_dev, sub, lane), n, 6).reshape(tok_dev, emb_dim)

        z_tgt = jnp.einsum('td,td->t', query_vec, tgt_rows, preferred_element_type=jnp.float32)
        z_cand = jnp.einsum('td,sd->ts', query_vec, cand_rows, preferred_element_type=jnp.float32) - cand_logq[None, :]
        z_cand = jnp.where(y_blk[:, None] == cand_ids[None, :], -1e9, z_cand)
        peak_val = jnp.maximum(jnp.max(z_cand, axis=1), z_tgt)
        exp_total = jnp.exp(z_tgt - peak_val) + jnp.sum(jnp.exp(z_cand - peak_val[:, None]), axis=1)
        log_norm = peak_val + jnp.log(exp_total)
        loss_part = jnp.sum(log_norm - z_tgt)
        dz_tgt = (jnp.exp(z_tgt - log_norm) - 1.0) / total_tok
        dz_cand = (jnp.exp(z_cand - log_norm[:, None]) / total_tok).astype(jnp.bfloat16)
        d_query = (dz_tgt[:, None] * tgt_rows.astype(jnp.float32)
                   + jnp.dot(dz_cand, cand_rows, preferred_element_type=jnp.float32)).astype(jnp.bfloat16)

        note = jnp.concatenate([dz_tgt, jnp.broadcast_to(loss_part, (8 * lane - tok_dev,))]).reshape(8, lane)
        notes = spread(note, n, 4).reshape(n, 8 * lane)
        loss_val = jnp.sum(notes[:, tok_dev]) / total_tok
        part_cand = jnp.einsum('ts,td->sd', dz_cand, query_vec, preferred_element_type=jnp.float32)
        own_cand_grad = reduce_scatter(part_cand, n, 1)
        sent_cand, query_all = lax.optimization_barrier((own_cand_grad.reshape(cand_dev, sub, lane), query_all))
        cand_grad = lax.all_gather(sent_cand, 'dp', tiled=True)

        part_two = jnp.einsum('tf,td->fd', hidden_act, d_query, preferred_element_type=jnp.float32)
        part_two, own_cand_grad = lax.optimization_barrier((part_two, own_cand_grad))
        own_two = reduce_scatter(part_two, n, 2)
        sent_two, cand_grad = lax.optimization_barrier((own_two, cand_grad))
        grad_two = lax.all_gather(sent_two, 'dp', tiled=True)

        d_act = jnp.einsum('td,fd->tf', d_query, w_two, preferred_element_type=jnp.float32)
        d_pre = gelu_back(d_act.astype(jnp.bfloat16).astype(jnp.float32))[0].astype(jnp.bfloat16)
        half = x_flip.shape[0] // 2
        low = outer(x_flip[:half], d_pre)
        low, own_two = lax.optimization_barrier((low, own_two))
        own_low = reduce_scatter(low, n, 3)
        sent_low, grad_two = lax.optimization_barrier((own_low, grad_two))
        all_low = lax.all_gather(sent_low, 'dp', tiled=True)
        high = outer(x_flip[half:], d_pre)
        high, own_low = lax.optimization_barrier((high, own_low))
        own_high = reduce_scatter(high, n, 7)
        sent_high, all_low = lax.optimization_barrier((own_high, all_low))
        all_high = lax.all_gather(sent_high, 'dp', tiled=True)
        grad_one = fill_high(fill_low(all_low), all_high)
        grad_two = carry_over(grad_two)

        grad_table = table_grad(keys, first, last, notes[:, :tok_dev].reshape(-1), query_all, cand_grad, rows_dev, n, count)
        return loss_val, grad_table, grad_one, grad_two

    return jax.shard_map(local_step, mesh=mesh,
                         in_specs=(P('dp', None), P(), P(), P('dp', None), P(), P(), P('dp')),
                         out_specs=(P(), P('dp', None), P(), P()), check_vma=False)
```

```python
import functools

import jax
import jax.numpy as jnp
from jax import lax
from jax.experimental import pallas as pl
from jax.experimental.pallas import tpu as pltpu
from jax.sharding import PartitionSpec as P

MESH = pl.DeviceIdType.MESH
PARTS = 8


def spread_kernel(n, in_ref, out_ref, send_sem, recv_sem):
    me = lax.axis_index('dp')
    barrier = pltpu.get_barrier_semaphore()

    def greet(i, carry):
        pl.semaphore_signal(barrier, inc=1, device_id=(lax.rem(me + i, n),), device_id_type=MESH)
        return carry

    lax.fori_loop(1, n, greet, 0)
    pl.semaphore_wait(barrier, n - 1)

    def send(i, carry):
        pltpu.make_async_remote_copy(
            src_ref=in_ref, dst_ref=out_ref.at[me], send_sem=send_sem, recv_sem=recv_sem,
            device_id=(lax.rem(me + i, n),), device_id_type=MESH).start()
        return carry

    lax.fori_loop(1, n, send, 0)
    others = out_ref.at[pl.ds(0, n - 1)]
    drain = pltpu.make_async_remote_copy(
        src_ref=others, dst_ref=others, send_sem=send_sem, recv_sem=recv_sem,
        device_id=(me,), device_id_type=MESH)
    drain.wait_recv()
    drain.wait_send()
    out_ref[me] = in_ref[...]


def spread(block, n, cid):
    return pl.pallas_call(
        functools.partial(spread_kernel, n),
        out_shape=jax.ShapeDtypeStruct((n,) + block.shape, block.dtype),
        in_specs=[pl.BlockSpec(memory_space=pltpu.VMEM)],
        out_specs=pl.BlockSpec(memory_space=pltpu.VMEM),
        scratch_shapes=[pltpu.SemaphoreType.DMA, pltpu.SemaphoreType.DMA],
        compiler_params=pltpu.CompilerParams(collective_id=cid, has_side_effects=True),
        name=f'spread_{cid}',
    )(block)


def reduce_kernel(tile, steps, in_ref, out_ref, fresh, held, *scratch):
    got, (load_sem, send_sem, recv_sem, store_sem) = scratch[:steps], scratch[steps:]
    me = lax.axis_index('dp')
    core = lax.rem(me, 2)
    xb, yb = lax.rem(me // 2, 2), lax.rem(me // 4, 2)
    z0, z1 = lax.rem(me // 8, 2), lax.rem(me // 16, 2)
    one = (1 + core, xb * (1 - core) + yb * core)
    two = (2 - core, yb * (1 - core) + xb * core)
    plain = (one, two, (4, z0), (8, z1))[:steps - 1]
    turned = ((4, z0), (8, z1), one, two) if steps > 4 else ((4, z0), one, two)

    def way(part):
        flip = (lax.rem(part, 4) + 3) // 4 * (1 - lax.rem(part, 4) // 2)
        return [(p + flip * (t - p), q + flip * (u - q)) for (p, q), (t, u) in zip(plain, turned)]

    def mate(step, part):
        if step == 0:
            return me + 1 - 2 * core
        weight, bit = way(part)[step - 1]
        return me + 2 * weight * (1 - 2 * bit)

    barrier = pltpu.get_barrier_semaphore()
    for step in range(steps):
        pl.semaphore_signal(barrier, inc=1, device_id=(mate(step, 0),), device_id_type=MESH)

    def piece(part):
        if tile[0] is None:
            return (slice(None), pl.ds(pl.multiple_of(part * tile[1], tile[1]), tile[1]))
        return (pl.ds(pl.multiple_of(part * tile[0], tile[0]), tile[0]),)

    def load(part):
        side = lax.rem(part, 2)
        return pltpu.make_async_copy(in_ref.at[(slice(None), core) + piece(part)], fresh.at[side], load_sem.at[side])

    load(0).start()
    pl.semaphore_wait(barrier, steps)

    def start_of(step, part, theirs):
        at = 0
        for k, (_, own) in enumerate(way(part)[:step]):
            bit = 1 - own if theirs and k == step - 1 else own
            at = at + bit * (1 << (steps - 2 - k))
        return at

    def send(step, part):
        if step == 0:
            source = in_ref.at[(slice(None), 1 - core) + piece(part)]
        else:
            source = held.at[part, pl.ds(start_of(step, part, True), got[step].shape[1])]
        pltpu.make_async_remote_copy(
            src_ref=source, dst_ref=got[step].at[part], send_sem=send_sem.at[step, part],
            recv_sem=recv_sem.at[step, part], device_id=(mate(step, part),), device_id_type=MESH).start()

    def landed(step, part):
        return pltpu.make_async_remote_copy(
            src_ref=got[step].at[part], dst_ref=got[step].at[part],
            send_sem=send_sem.at[step, part], recv_sem=recv_sem.at[step, part],
            device_id=(mate(step, part),), device_id_type=MESH)

    def add(step, part):
        dims = way(part)
        start = start_of(step, part, False)

        def one(i, carry):
            if step == 0:
                at = 0
                for k, (weight, _) in enumerate(dims):
                    at = at + lax.rem(i // weight, 2) * (1 << (steps - 2 - k))
                held[part, at] = fresh[lax.rem(part, 2), i] + got[0][part, i]
            else:
                held[part, start + i] = held[part, start + i] + got[step][part, i]
            return carry
        lax.fori_loop(0, got[step].shape[1], one, 0)

    def store(part):
        return pltpu.make_async_copy(held.at[part, start_of(steps - 1, part, False)], out_ref.at[piece(part)],
                                     store_sem.at[part])

    def tick(t, carry):
        @pl.when(t < PARTS)
        def _():
            send(0, t)

        for step in range(steps):
            part = t - 1 - step

            @pl.when((part >= 0) & (part < PARTS))
            def _():
                if step == 0:
                    load(part).wait()

                    @pl.when(part + 1 < PARTS)
                    def _():
                        load(part + 1).start()
                landed(step, part).wait_recv()
                add(step, part)
                if step < steps - 1:
                    send(step + 1, part)
                else:
                    store(part).start()

        return carry

    lax.fori_loop(0, PARTS + steps, tick, 0)

    def finish(part, carry):
        for step in range(steps):
            landed(step, part).wait_send()
        store(part).wait()
        return carry

    lax.fori_loop(0, PARTS, finish, 0)


def reduce_scatter(x, n, cid):
    per, rest = x.shape[0] // n, x.shape[1:]
    if len(rest) == 2 or per // PARTS >= 8:
        tile, piece = (per // PARTS, None), (per // PARTS,) + rest
    else:
        tile, piece = (None, rest[0] // PARTS), (per, rest[0] // PARTS)
    steps = n.bit_length() - 1
    got = [pltpu.VMEM((PARTS, n >> (s + 1)) + piece, x.dtype) for s in range(steps)]
    size = x.size * x.dtype.itemsize
    return pl.pallas_call(
        functools.partial(reduce_kernel, tile, steps),
        out_shape=jax.ShapeDtypeStruct((per,) + rest, x.dtype),
        in_specs=[pl.BlockSpec(memory_space=pl.ANY)],
        out_specs=pl.BlockSpec(memory_space=pl.ANY),
        scratch_shapes=[pltpu.VMEM((2, n // 2) + piece, x.dtype), pltpu.VMEM((PARTS, n // 2) + piece, x.dtype)] + got + [
            pltpu.SemaphoreType.DMA((2,)),
            pltpu.SemaphoreType.DMA((steps, PARTS)),
            pltpu.SemaphoreType.DMA((steps, PARTS)),
            pltpu.SemaphoreType.DMA((PARTS,)),
        ],
        compiler_params=pltpu.CompilerParams(collective_id=cid, has_side_effects=True,
                                             vmem_limit_bytes=min(size * 7 // 4 + 4 * 2**20, 67043328)),
        name=f'reduce_{cid}',
    )(x.reshape((n // 2, 2, per) + rest))


SLOT_BITS = 1024
OUT_ROWS = 256


def pick_kernel(n, count, rows_dev, keys, first, last, table, tgt_out, cand_out, buf, sems):
    base = lax.axis_index('dp') * rows_dev
    tok_dev = tgt_out.shape[1]

    def zero(i, carry):
        for side in range(2):
            buf[side, pl.ds(i * 32, 32)] = jnp.zeros((32,) + buf.shape[2:], buf.dtype)
        return carry

    lax.fori_loop(0, count // 32, zero, 0)

    def out_copies(j, side):
        return (pltpu.make_async_copy(buf.at[side, pl.ds(0, tok_dev)], tgt_out.at[j], sems.at[side, 0]),
                pltpu.make_async_copy(buf.at[side, pl.ds(tok_dev, count - tok_dev)], cand_out.at[j], sems.at[side, 1]))

    def per_dev(j, carry):
        side = lax.rem(j, 2)

        @pl.when(j >= 2)
        def _():
            for copy in out_copies(j - 2, side):
                copy.wait()

            def clear(i, c):
                buf[side, lax.rem(keys[(j - 2) * count + i], SLOT_BITS)] = jnp.zeros(buf.shape[2:], buf.dtype)
                return c

            lax.fori_loop(first[j - 2], last[j - 2], clear, 0)

        def one(i, c):
            key = keys[j * count + i]
            buf[side, lax.rem(key, SLOT_BITS)] = table[key // SLOT_BITS - base]
            return c

        lax.fori_loop(first[j], last[j], one, 0)
        for copy in out_copies(j, side):
            copy.start()
        return carry

    lax.fori_loop(0, n, per_dev, 0)
    for copy in out_copies(n - 2, 0) + out_copies(n - 1, 1):
        copy.wait()


def pick_rows(table3, keys, first, last, n, count, tok_dev):
    smem = pl.BlockSpec(memory_space=pltpu.SMEM)
    anywhere = pl.BlockSpec(memory_space=pl.ANY)
    tail = table3.shape[1:]
    return pl.pallas_call(
        functools.partial(pick_kernel, n, count, table3.shape[0]),
        out_shape=(jax.ShapeDtypeStruct((n, tok_dev) + tail, table3.dtype),
                   jax.ShapeDtypeStruct((n, count - tok_dev) + tail, table3.dtype)),
        in_specs=[smem, smem, smem, pl.BlockSpec(memory_space=pltpu.VMEM)],
        out_specs=(anywhere, anywhere),
        scratch_shapes=[pltpu.VMEM((2, count) + tail, table3.dtype), pltpu.SemaphoreType.DMA((2, 2))],
        compiler_params=pltpu.CompilerParams(vmem_limit_bytes=24 * 2**20),
        name='pick_rows',
    )(keys, first, last, table3)


def table_kernel(n, count, tok_dev, rows_dev, lane, keys, first, last, scale, query, cand, out_ref, acc):
    step = pl.program_id(0)
    base = lax.axis_index('dp') * rows_dev

    @pl.when(step == 0)
    def _():
        def zero(i, carry):
            acc[pl.ds(i * 64, 64)] = jnp.zeros((64,) + acc.shape[1:], jnp.float32)
            return carry

        lax.fori_loop(0, rows_dev // 64, zero, 0)

    @pl.when(step < n)
    def _():
        def one(i, carry):
            key = keys[step * count + i]
            at = key // SLOT_BITS - base
            slot = lax.rem(key, SLOT_BITS)

            @pl.when(slot < tok_dev)
            def _():
                acc[at] = acc[at] + scale[step * tok_dev + slot] * query[slot].astype(jnp.float32)

            @pl.when(slot >= tok_dev)
            def _():
                acc[at] = acc[at] + cand[slot - tok_dev]

            return carry

        lax.fori_loop(first[step], last[step], one, 0)

    @pl.when(step >= n)
    def _():
        for j in range(acc.shape[1]):
            out_ref[:, j * lane:(j + 1) * lane] = acc[pl.ds((step - n) * OUT_ROWS, OUT_ROWS), j, :]


def table_grad(keys, first, last, scale, query, cand, rows_dev, n, count):
    tok_dev, cand_dev = query.shape[0] // n, cand.shape[0] // n
    sub, lane = query.shape[1:]
    smem = pl.BlockSpec(memory_space=pltpu.SMEM)
    size = 4 * rows_dev * sub * lane
    return pl.pallas_call(
        functools.partial(table_kernel, n, count, tok_dev, rows_dev, lane),
        grid=(n + rows_dev // OUT_ROWS,),
        out_shape=jax.ShapeDtypeStruct((rows_dev, sub * lane), jnp.float32),
        in_specs=[smem, smem, smem, smem,
                  pl.BlockSpec((tok_dev, sub, lane), lambda i: (jnp.minimum(i, n - 1), 0, 0)),
                  pl.BlockSpec((cand_dev, sub, lane), lambda i: (jnp.minimum(i, n - 1), 0, 0))],
        out_specs=pl.BlockSpec((OUT_ROWS, sub * lane), lambda i: (jnp.maximum(i - n, 0), 0)),
        scratch_shapes=[pltpu.VMEM((rows_dev, sub, lane), jnp.float32)],
        cost_estimate=pl.CostEstimate(flops=30_000_000_000, bytes_accessed=4 * size, transcendentals=0),
        compiler_params=pltpu.CompilerParams(vmem_limit_bytes=size + 12 * 2**20),
        name='table_grad',
    )(keys, first, last, scale, query, cand)


def outer_kernel(left, right, out_ref):
    out_ref[...] = jnp.dot(left[...], right[...], preferred_element_type=jnp.float32)


def outer(left, right):
    rows, depth = left.shape
    cols = right.shape[1]
    high, wide = rows, cols // 8
    return pl.pallas_call(
        outer_kernel,
        grid=(rows // high, cols // wide),
        out_shape=jax.ShapeDtypeStruct((rows, cols), jnp.float32),
        in_specs=[pl.BlockSpec((high, depth), lambda i, j: (i, 0)), pl.BlockSpec((depth, wide), lambda i, j: (0, j))],
        out_specs=pl.BlockSpec((high, wide), lambda i, j: (i, j)),
        cost_estimate=pl.CostEstimate(flops=2 * rows * cols * depth, bytes_accessed=4 * rows * cols, transcendentals=0),
        compiler_params=pltpu.CompilerParams(vmem_limit_bytes=16 * 2**20),
        name='outer',
    )(left, right)


def carry_kernel(in_ref, out_ref):
    out_ref[...] = in_ref[...]


def carry_over(x):
    rows, cols = x.shape
    spec = pl.BlockSpec((rows // 8, cols), lambda i: (i, 0))
    return pl.pallas_call(
        carry_kernel, grid=(8,), out_shape=jax.ShapeDtypeStruct(x.shape, x.dtype), in_specs=[spec], out_specs=spec,
        cost_estimate=pl.CostEstimate(flops=x.size, bytes_accessed=8 * x.size, transcendentals=0),
        compiler_params=pltpu.CompilerParams(vmem_limit_bytes=16 * 2**20), name='carry_over')(x)


def solution(mesh):
    n = mesh.shape['dp']

    def local_step(x_blk, w_one, w_two, table_blk, cand_ids, cand_logq, y_blk):
        tok_dev = x_blk.shape[0]
        rows_dev, emb_dim = table_blk.shape
        total_tok = tok_dev * n
        cand_dev = cand_ids.shape[0] // n
        count = tok_dev + cand_dev
        lane = 128
        sub = emb_dim // lane
        me = lax.axis_index('dp')

        slots = jnp.arange(count, dtype=jnp.int32)
        wants = jnp.concatenate([y_blk, lax.dynamic_slice(cand_ids, (me * cand_dev,), (cand_dev,))]) * SLOT_BITS + slots
        rank = jnp.sum((wants[None, :] < wants[:, None]).astype(jnp.int32), axis=1)
        sorted_own = jnp.sum(jnp.where(rank[:, None] == slots[None, :], wants[:, None], 0), axis=0)
        block = jnp.pad(sorted_own, (0, (-count) % (8 * lane))).reshape(-1, lane)
        everyone = spread(block, n, 0).reshape(n, -1)[:, :count]
        first = jnp.sum((everyone < me * rows_dev * SLOT_BITS).astype(jnp.int32), axis=1)
        last = jnp.sum((everyone - me * rows_dev * SLOT_BITS < rows_dev * SLOT_BITS).astype(jnp.int32), axis=1)
        keys = everyone.reshape(-1)

        tgt_part, cand_part = pick_rows(table_blk.reshape(rows_dev, sub, lane), keys, first, last, n, count, tok_dev)
        own_cand = reduce_scatter(cand_part.reshape(n * cand_dev, sub, lane), n, 5).reshape(cand_dev, emb_dim)
        cand_rows = lax.all_gather(own_cand, 'dp', tiled=True)

        x_flip = lax.optimization_barrier(x_blk.T)
        pre_act = jnp.dot(x_blk, w_one, preferred_element_type=jnp.float32).astype(jnp.bfloat16)
        act_val, gelu_back = jax.vjp(jax.nn.gelu, pre_act.astype(jnp.float32))
        hidden_act = act_val.astype(jnp.bfloat16)
        query_vec = jnp.dot(hidden_act, w_two, preferred_element_type=jnp.float32).astype(jnp.bfloat16)
        query_all = lax.all_gather(query_vec.reshape(tok_dev, sub, lane), 'dp', tiled=True)
        tgt_part, query_vec = lax.optimization_barrier((tgt_part, query_vec))
        tgt_rows = reduce_scatter(tgt_part.reshape(n * tok_dev, sub, lane), n, 6).reshape(tok_dev, emb_dim)

        z_tgt = jnp.einsum('td,td->t', query_vec, tgt_rows, preferred_element_type=jnp.float32)
        z_cand = jnp.einsum('td,sd->ts', query_vec, cand_rows, preferred_element_type=jnp.float32) - cand_logq[None, :]
        z_cand = jnp.where(y_blk[:, None] == cand_ids[None, :], -1e9, z_cand)
        peak_val = jnp.maximum(jnp.max(z_cand, axis=1), z_tgt)
        exp_total = jnp.exp(z_tgt - peak_val) + jnp.sum(jnp.exp(z_cand - peak_val[:, None]), axis=1)
        log_norm = peak_val + jnp.log(exp_total)
        loss_part = jnp.sum(log_norm - z_tgt)
        dz_tgt = (jnp.exp(z_tgt - log_norm) - 1.0) / total_tok
        dz_cand = (jnp.exp(z_cand - log_norm[:, None]) / total_tok).astype(jnp.bfloat16)
        d_query = (dz_tgt[:, None] * tgt_rows.astype(jnp.float32)
                   + jnp.dot(dz_cand, cand_rows, preferred_element_type=jnp.float32)).astype(jnp.bfloat16)

        note = jnp.concatenate([dz_tgt, jnp.broadcast_to(loss_part, (8 * lane - tok_dev,))]).reshape(8, lane)
        notes = spread(note, n, 4).reshape(n, 8 * lane)
        loss_val = jnp.sum(notes[:, tok_dev]) / total_tok
        part_cand = jnp.einsum('ts,td->sd', dz_cand, query_vec, preferred_element_type=jnp.float32)
        own_cand_grad = reduce_scatter(part_cand, n, 1)
        sent_cand, query_all = lax.optimization_barrier((own_cand_grad.reshape(cand_dev, sub, lane), query_all))
        cand_grad = lax.all_gather(sent_cand, 'dp', tiled=True)

        part_two = jnp.einsum('tf,td->fd', hidden_act, d_query, preferred_element_type=jnp.float32)
        part_two, own_cand_grad = lax.optimization_barrier((part_two, own_cand_grad))
        own_two = reduce_scatter(part_two, n, 2)
        sent_two, cand_grad = lax.optimization_barrier((own_two, cand_grad))
        grad_two = lax.all_gather(sent_two, 'dp', tiled=True)

        d_act = jnp.einsum('td,fd->tf', d_query, w_two, preferred_element_type=jnp.float32)
        d_pre = gelu_back(d_act.astype(jnp.bfloat16).astype(jnp.float32))[0].astype(jnp.bfloat16)
        part_one = outer(x_flip, d_pre)
        part_one, own_two = lax.optimization_barrier((part_one, own_two))
        own_one = reduce_scatter(part_one, n, 3)
        sent_one, grad_two = lax.optimization_barrier((own_one, grad_two))
        grad_one = carry_over(lax.all_gather(sent_one, 'dp', tiled=True))
        grad_two = carry_over(grad_two)

        grad_table = table_grad(keys, first, last, notes[:, :tok_dev].reshape(-1), query_all, cand_grad, rows_dev, n, count)
        return loss_val, grad_table, grad_one, grad_two

    return jax.shard_map(local_step, mesh=mesh,
                         in_specs=(P('dp', None), P(), P(), P('dp', None), P(), P(), P('dp')),
                         out_specs=(P(), P('dp', None), P(), P()), check_vma=False)
```

```python
import functools

import jax
import jax.numpy as jnp
from jax import lax
from jax.experimental import pallas as pl
from jax.experimental.pallas import tpu as pltpu
from jax.sharding import PartitionSpec as P

MESH = pl.DeviceIdType.MESH
PARTS = 8


def spread_kernel(n, in_ref, out_ref, send_sem, recv_sem):
    me = lax.axis_index('dp')
    barrier = pltpu.get_barrier_semaphore()

    def greet(i, carry):
        pl.semaphore_signal(barrier, inc=1, device_id=(lax.rem(me + i, n),), device_id_type=MESH)
        return carry

    lax.fori_loop(1, n, greet, 0)
    pl.semaphore_wait(barrier, n - 1)

    def send(i, carry):
        pltpu.make_async_remote_copy(
            src_ref=in_ref, dst_ref=out_ref.at[me], send_sem=send_sem, recv_sem=recv_sem,
            device_id=(lax.rem(me + i, n),), device_id_type=MESH).start()
        return carry

    lax.fori_loop(1, n, send, 0)
    others = out_ref.at[pl.ds(0, n - 1)]
    drain = pltpu.make_async_remote_copy(
        src_ref=others, dst_ref=others, send_sem=send_sem, recv_sem=recv_sem,
        device_id=(me,), device_id_type=MESH)
    drain.wait_recv()
    drain.wait_send()
    out_ref[me] = in_ref[...]


def spread(block, n, cid):
    return pl.pallas_call(
        functools.partial(spread_kernel, n),
        out_shape=jax.ShapeDtypeStruct((n,) + block.shape, block.dtype),
        in_specs=[pl.BlockSpec(memory_space=pltpu.VMEM)],
        out_specs=pl.BlockSpec(memory_space=pltpu.VMEM),
        scratch_shapes=[pltpu.SemaphoreType.DMA, pltpu.SemaphoreType.DMA],
        compiler_params=pltpu.CompilerParams(collective_id=cid, has_side_effects=True),
        name=f'spread_{cid}',
    )(block)


def reduce_kernel(tile, steps, in_ref, out_ref, fresh, held, *scratch):
    got, (load_sem, send_sem, recv_sem, store_sem) = scratch[:steps], scratch[steps:]
    me = lax.axis_index('dp')
    core = lax.rem(me, 2)
    xb, yb = lax.rem(me // 2, 2), lax.rem(me // 4, 2)
    z0, z1 = lax.rem(me // 8, 2), lax.rem(me // 16, 2)
    one = (1 + core, xb * (1 - core) + yb * core)
    two = (2 - core, yb * (1 - core) + xb * core)
    plain = (one, two, (4, z0), (8, z1))[:steps - 1]
    turned = ((4, z0), (8, z1), one, two) if steps > 4 else ((4, z0), one, two)

    def way(part):
        flip = (lax.rem(part, 4) + 3) // 4 * (1 - lax.rem(part, 4) // 2)
        return [(p + flip * (t - p), q + flip * (u - q)) for (p, q), (t, u) in zip(plain, turned)]

    def mate(step, part):
        if step == 0:
            return me + 1 - 2 * core
        weight, bit = way(part)[step - 1]
        return me + 2 * weight * (1 - 2 * bit)

    barrier = pltpu.get_barrier_semaphore()
    for step in range(steps):
        pl.semaphore_signal(barrier, inc=1, device_id=(mate(step, 0),), device_id_type=MESH)

    def piece(part):
        if tile[0] is None:
            return (slice(None), pl.ds(pl.multiple_of(part * tile[1], tile[1]), tile[1]))
        return (pl.ds(pl.multiple_of(part * tile[0], tile[0]), tile[0]),)

    def load(part):
        side = lax.rem(part, 2)
        return pltpu.make_async_copy(in_ref.at[(slice(None), slice(None)) + piece(part)], fresh.at[side], load_sem.at[side])

    load(0).start()
    load(1).start()
    pl.semaphore_wait(barrier, steps)

    def start_of(step, part, theirs):
        at = 0
        for k, (_, own) in enumerate(way(part)[:step]):
            bit = 1 - own if theirs and k == step - 1 else own
            at = at + bit * (1 << (steps - 2 - k))
        return at

    def send(step, part):
        if step == 0:
            group = got[0].shape[1] // 4
            for k in range(4):
                run = pl.ds(k * group, group)
                pltpu.make_async_remote_copy(
                    src_ref=fresh.at[lax.rem(part, 2), run, 1 - core], dst_ref=got[0].at[part, run],
                    send_sem=send_sem.at[0, part], recv_sem=recv_sem.at[0, part],
                    device_id=(mate(0, part),), device_id_type=MESH).start()
            return
        source = held.at[part, pl.ds(start_of(step, part, True), got[step].shape[1])]
        pltpu.make_async_remote_copy(
            src_ref=source, dst_ref=got[step].at[part], send_sem=send_sem.at[step, part],
            recv_sem=recv_sem.at[step, part], device_id=(mate(step, part),), device_id_type=MESH).start()

    def landed(step, part):
        return pltpu.make_async_remote_copy(
            src_ref=got[step].at[part], dst_ref=got[step].at[part],
            send_sem=send_sem.at[step, part], recv_sem=recv_sem.at[step, part],
            device_id=(mate(step, part),), device_id_type=MESH)

    def add(step, part):
        dims = way(part)
        start = start_of(step, part, False)

        def one(i, carry):
            if step == 0:
                at = 0
                for k, (weight, _) in enumerate(dims):
                    at = at + lax.rem(i // weight, 2) * (1 << (steps - 2 - k))
                held[part, at] = fresh[lax.rem(part, 2), i, core] + got[0][part, i]
            else:
                held[part, start + i] = held[part, start + i] + got[step][part, i]
            return carry
        lax.fori_loop(0, got[step].shape[1], one, 0)

    def store(part):
        return pltpu.make_async_copy(held.at[part, start_of(steps - 1, part, False)], out_ref.at[piece(part)],
                                     store_sem.at[part])

    def tick(t, carry):
        @pl.when(t < PARTS)
        def _():
            load(t).wait()
            send(0, t)

        for step in range(steps):
            part = t - 1 - step

            @pl.when((part >= 0) & (part < PARTS))
            def _():
                landed(step, part).wait_recv()
                add(step, part)
                if step < steps - 1:
                    send(step + 1, part)
                else:
                    store(part).start()
                if step == 0:
                    landed(0, part).wait_send()

                    @pl.when(part + 2 < PARTS)
                    def _():
                        load(part + 2).start()

        return carry

    lax.fori_loop(0, PARTS + steps, tick, 0)

    def finish(part, carry):
        for step in range(1, steps):
            landed(step, part).wait_send()
        store(part).wait()
        return carry

    lax.fori_loop(0, PARTS, finish, 0)


def reduce_scatter(x, n, cid):
    per, rest = x.shape[0] // n, x.shape[1:]
    if len(rest) == 2 or per // PARTS >= 8:
        tile, piece = (per // PARTS, None), (per // PARTS,) + rest
    else:
        tile, piece = (None, rest[0] // PARTS), (per, rest[0] // PARTS)
    steps = n.bit_length() - 1
    got = [pltpu.VMEM((PARTS, n >> (s + 1)) + piece, x.dtype) for s in range(steps)]
    size = x.size * x.dtype.itemsize
    return pl.pallas_call(
        functools.partial(reduce_kernel, tile, steps),
        out_shape=jax.ShapeDtypeStruct((per,) + rest, x.dtype),
        in_specs=[pl.BlockSpec(memory_space=pl.ANY)],
        out_specs=pl.BlockSpec(memory_space=pl.ANY),
        scratch_shapes=[pltpu.VMEM((2, n // 2, 2) + piece, x.dtype), pltpu.VMEM((PARTS, n // 2) + piece, x.dtype)] + got + [
            pltpu.SemaphoreType.DMA((2,)),
            pltpu.SemaphoreType.DMA((steps, PARTS)),
            pltpu.SemaphoreType.DMA((steps, PARTS)),
            pltpu.SemaphoreType.DMA((PARTS,)),
        ],
        compiler_params=pltpu.CompilerParams(collective_id=cid, has_side_effects=True,
                                             vmem_limit_bytes=min(size * 15 // 8 + 4 * 2**20, 67043328)),
        name=f'reduce_{cid}',
    )(x.reshape((n // 2, 2, per) + rest))


SLOT_BITS = 1024
OUT_ROWS = 256


def pick_kernel(n, count, rows_dev, keys, first, last, table, tgt_out, cand_out, buf, sems):
    base = lax.axis_index('dp') * rows_dev
    tok_dev = tgt_out.shape[1]

    def zero(i, carry):
        for side in range(2):
            buf[side, pl.ds(i * 32, 32)] = jnp.zeros((32,) + buf.shape[2:], buf.dtype)
        return carry

    lax.fori_loop(0, count // 32, zero, 0)

    def out_copies(j, side):
        return (pltpu.make_async_copy(buf.at[side, pl.ds(0, tok_dev)], tgt_out.at[j], sems.at[side, 0]),
                pltpu.make_async_copy(buf.at[side, pl.ds(tok_dev, count - tok_dev)], cand_out.at[j], sems.at[side, 1]))

    def per_dev(j, carry):
        side = lax.rem(j, 2)

        @pl.when(j >= 2)
        def _():
            for copy in out_copies(j - 2, side):
                copy.wait()

            def clear(i, c):
                buf[side, lax.rem(keys[(j - 2) * count + i], SLOT_BITS)] = jnp.zeros(buf.shape[2:], buf.dtype)
                return c

            lax.fori_loop(first[j - 2], last[j - 2], clear, 0)

        def one(i, c):
            key = keys[j * count + i]
            buf[side, lax.rem(key, SLOT_BITS)] = table[key // SLOT_BITS - base]
            return c

        lax.fori_loop(first[j], last[j], one, 0)
        for copy in out_copies(j, side):
            copy.start()
        return carry

    lax.fori_loop(0, n, per_dev, 0)
    for copy in out_copies(n - 2, 0) + out_copies(n - 1, 1):
        copy.wait()


def pick_rows(table3, keys, first, last, n, count, tok_dev):
    smem = pl.BlockSpec(memory_space=pltpu.SMEM)
    anywhere = pl.BlockSpec(memory_space=pl.ANY)
    tail = table3.shape[1:]
    return pl.pallas_call(
        functools.partial(pick_kernel, n, count, table3.shape[0]),
        out_shape=(jax.ShapeDtypeStruct((n, tok_dev) + tail, table3.dtype),
                   jax.ShapeDtypeStruct((n, count - tok_dev) + tail, table3.dtype)),
        in_specs=[smem, smem, smem, pl.BlockSpec(memory_space=pltpu.VMEM)],
        out_specs=(anywhere, anywhere),
        scratch_shapes=[pltpu.VMEM((2, count) + tail, table3.dtype), pltpu.SemaphoreType.DMA((2, 2))],
        compiler_params=pltpu.CompilerParams(vmem_limit_bytes=24 * 2**20),
        name='pick_rows',
    )(keys, first, last, table3)


def table_kernel(n, count, tok_dev, rows_dev, lane, keys, first, last, scale, query, cand, out_ref, acc):
    step = pl.program_id(0)
    base = lax.axis_index('dp') * rows_dev

    @pl.when(step == 0)
    def _():
        def zero(i, carry):
            acc[pl.ds(i * 64, 64)] = jnp.zeros((64,) + acc.shape[1:], jnp.float32)
            return carry

        lax.fori_loop(0, rows_dev // 64, zero, 0)

    @pl.when(step < n)
    def _():
        def one(i, carry):
            key = keys[step * count + i]
            at = key // SLOT_BITS - base
            slot = lax.rem(key, SLOT_BITS)

            @pl.when(slot < tok_dev)
            def _():
                acc[at] = acc[at] + scale[step * tok_dev + slot] * query[slot].astype(jnp.float32)

            @pl.when(slot >= tok_dev)
            def _():
                acc[at] = acc[at] + cand[slot - tok_dev]

            return carry

        lax.fori_loop(first[step], last[step], one, 0)

    @pl.when(step >= n)
    def _():
        for j in range(acc.shape[1]):
            out_ref[:, j * lane:(j + 1) * lane] = acc[pl.ds((step - n) * OUT_ROWS, OUT_ROWS), j, :]


def table_grad(keys, first, last, scale, query, cand, rows_dev, n, count):
    tok_dev, cand_dev = query.shape[0] // n, cand.shape[0] // n
    sub, lane = query.shape[1:]
    smem = pl.BlockSpec(memory_space=pltpu.SMEM)
    size = 4 * rows_dev * sub * lane
    return pl.pallas_call(
        functools.partial(table_kernel, n, count, tok_dev, rows_dev, lane),
        grid=(n + rows_dev // OUT_ROWS,),
        out_shape=jax.ShapeDtypeStruct((rows_dev, sub * lane), jnp.float32),
        in_specs=[smem, smem, smem, smem,
                  pl.BlockSpec((tok_dev, sub, lane), lambda i: (jnp.minimum(i, n - 1), 0, 0)),
                  pl.BlockSpec((cand_dev, sub, lane), lambda i: (jnp.minimum(i, n - 1), 0, 0))],
        out_specs=pl.BlockSpec((OUT_ROWS, sub * lane), lambda i: (jnp.maximum(i - n, 0), 0)),
        scratch_shapes=[pltpu.VMEM((rows_dev, sub, lane), jnp.float32)],
        cost_estimate=pl.CostEstimate(flops=30_000_000_000, bytes_accessed=4 * size, transcendentals=0),
        compiler_params=pltpu.CompilerParams(vmem_limit_bytes=size + 12 * 2**20),
        name='table_grad',
    )(keys, first, last, scale, query, cand)


def outer_kernel(left, right, out_ref):
    out_ref[...] = jnp.dot(left[...], right[...], preferred_element_type=jnp.float32)


def outer(left, right):
    rows, depth = left.shape
    cols = right.shape[1]
    high, wide = rows, cols // 8
    return pl.pallas_call(
        outer_kernel,
        grid=(rows // high, cols // wide),
        out_shape=jax.ShapeDtypeStruct((rows, cols), jnp.float32),
        in_specs=[pl.BlockSpec((high, depth), lambda i, j: (i, 0)), pl.BlockSpec((depth, wide), lambda i, j: (0, j))],
        out_specs=pl.BlockSpec((high, wide), lambda i, j: (i, j)),
        cost_estimate=pl.CostEstimate(flops=2 * rows * cols * depth, bytes_accessed=4 * rows * cols, transcendentals=0),
        compiler_params=pltpu.CompilerParams(vmem_limit_bytes=16 * 2**20),
        name='outer',
    )(left, right)


def carry_kernel(in_ref, out_ref):
    out_ref[...] = in_ref[...]


def carry_over(x):
    rows, cols = x.shape
    spec = pl.BlockSpec((rows // 8, cols), lambda i: (i, 0))
    return pl.pallas_call(
        carry_kernel, grid=(8,), out_shape=jax.ShapeDtypeStruct(x.shape, x.dtype), in_specs=[spec], out_specs=spec,
        cost_estimate=pl.CostEstimate(flops=x.size, bytes_accessed=8 * x.size, transcendentals=0),
        compiler_params=pltpu.CompilerParams(vmem_limit_bytes=16 * 2**20), name='carry_over')(x)


def solution(mesh):
    n = mesh.shape['dp']

    def local_step(x_blk, w_one, w_two, table_blk, cand_ids, cand_logq, y_blk):
        tok_dev = x_blk.shape[0]
        rows_dev, emb_dim = table_blk.shape
        total_tok = tok_dev * n
        cand_dev = cand_ids.shape[0] // n
        count = tok_dev + cand_dev
        lane = 128
        sub = emb_dim // lane
        me = lax.axis_index('dp')

        slots = jnp.arange(count, dtype=jnp.int32)
        wants = jnp.concatenate([y_blk, lax.dynamic_slice(cand_ids, (me * cand_dev,), (cand_dev,))]) * SLOT_BITS + slots
        rank = jnp.sum((wants[None, :] < wants[:, None]).astype(jnp.int32), axis=1)
        sorted_own = jnp.sum(jnp.where(rank[:, None] == slots[None, :], wants[:, None], 0), axis=0)
        block = jnp.pad(sorted_own, (0, (-count) % (8 * lane))).reshape(-1, lane)
        everyone = spread(block, n, 0).reshape(n, -1)[:, :count]
        first = jnp.sum((everyone < me * rows_dev * SLOT_BITS).astype(jnp.int32), axis=1)
        last = jnp.sum((everyone - me * rows_dev * SLOT_BITS < rows_dev * SLOT_BITS).astype(jnp.int32), axis=1)
        keys = everyone.reshape(-1)

        tgt_part, cand_part = pick_rows(table_blk.reshape(rows_dev, sub, lane), keys, first, last, n, count, tok_dev)
        own_cand = reduce_scatter(cand_part.reshape(n * cand_dev, sub, lane), n, 5).reshape(cand_dev, emb_dim)
        cand_rows = lax.all_gather(own_cand, 'dp', tiled=True)

        x_flip = lax.optimization_barrier(x_blk.T)
        pre_act = jnp.dot(x_blk, w_one, preferred_element_type=jnp.float32).astype(jnp.bfloat16)
        act_val, gelu_back = jax.vjp(jax.nn.gelu, pre_act.astype(jnp.float32))
        hidden_act = act_val.astype(jnp.bfloat16)
        query_vec = jnp.dot(hidden_act, w_two, preferred_element_type=jnp.float32).astype(jnp.bfloat16)
        query_all = lax.all_gather(query_vec.reshape(tok_dev, sub, lane), 'dp', tiled=True)
        tgt_part, query_vec = lax.optimization_barrier((tgt_part, query_vec))
        tgt_rows = reduce_scatter(tgt_part.reshape(n * tok_dev, sub, lane), n, 6).reshape(tok_dev, emb_dim)

        z_tgt = jnp.einsum('td,td->t', query_vec, tgt_rows, preferred_element_type=jnp.float32)
        z_cand = jnp.einsum('td,sd->ts', query_vec, cand_rows, preferred_element_type=jnp.float32) - cand_logq[None, :]
        z_cand = jnp.where(y_blk[:, None] == cand_ids[None, :], -1e9, z_cand)
        peak_val = jnp.maximum(jnp.max(z_cand, axis=1), z_tgt)
        exp_total = jnp.exp(z_tgt - peak_val) + jnp.sum(jnp.exp(z_cand - peak_val[:, None]), axis=1)
        log_norm = peak_val + jnp.log(exp_total)
        loss_part = jnp.sum(log_norm - z_tgt)
        dz_tgt = (jnp.exp(z_tgt - log_norm) - 1.0) / total_tok
        dz_cand = (jnp.exp(z_cand - log_norm[:, None]) / total_tok).astype(jnp.bfloat16)
        d_query = (dz_tgt[:, None] * tgt_rows.astype(jnp.float32)
                   + jnp.dot(dz_cand, cand_rows, preferred_element_type=jnp.float32)).astype(jnp.bfloat16)

        note = jnp.concatenate([dz_tgt, jnp.broadcast_to(loss_part, (8 * lane - tok_dev,))]).reshape(8, lane)
        notes = spread(note, n, 4).reshape(n, 8 * lane)
        loss_val = jnp.sum(notes[:, tok_dev]) / total_tok
        part_cand = jnp.einsum('ts,td->sd', dz_cand, query_vec, preferred_element_type=jnp.float32)
        own_cand_grad = reduce_scatter(part_cand, n, 1)
        sent_cand, query_all = lax.optimization_barrier((own_cand_grad.reshape(cand_dev, sub, lane), query_all))
        cand_grad = lax.all_gather(sent_cand, 'dp', tiled=True)

        part_two = jnp.einsum('tf,td->fd', hidden_act, d_query, preferred_element_type=jnp.float32)
        part_two, own_cand_grad = lax.optimization_barrier((part_two, own_cand_grad))
        own_two = reduce_scatter(part_two, n, 2)
        sent_two, cand_grad = lax.optimization_barrier((own_two, cand_grad))
        grad_two = lax.all_gather(sent_two, 'dp', tiled=True)

        d_act = jnp.einsum('td,fd->tf', d_query, w_two, preferred_element_type=jnp.float32)
        d_pre = gelu_back(d_act.astype(jnp.bfloat16).astype(jnp.float32))[0].astype(jnp.bfloat16)
        part_one = outer(x_flip, d_pre)
        part_one, own_two = lax.optimization_barrier((part_one, own_two))
        own_one = reduce_scatter(part_one, n, 3)
        sent_one, grad_two = lax.optimization_barrier((own_one, grad_two))
        grad_one = carry_over(lax.all_gather(sent_one, 'dp', tiled=True))
        grad_two = carry_over(grad_two)

        grad_table = table_grad(keys, first, last, notes[:, :tok_dev].reshape(-1), query_all, cand_grad, rows_dev, n, count)
        return loss_val, grad_table, grad_one, grad_two

    return jax.shard_map(local_step, mesh=mesh,
                         in_specs=(P('dp', None), P(), P(), P('dp', None), P(), P(), P('dp')),
                         out_specs=(P(), P('dp', None), P(), P()), check_vma=False)
```

```python
import functools

import jax
import jax.numpy as jnp
from jax import lax
from jax.experimental import pallas as pl
from jax.experimental.pallas import tpu as pltpu
from jax.sharding import PartitionSpec as P

MESH = pl.DeviceIdType.MESH
PARTS = 8


def spread_kernel(n, in_ref, out_ref, send_sem, recv_sem):
    me = lax.axis_index('dp')
    barrier = pltpu.get_barrier_semaphore()

    def greet(i, carry):
        pl.semaphore_signal(barrier, inc=1, device_id=(lax.rem(me + i, n),), device_id_type=MESH)
        return carry

    lax.fori_loop(1, n, greet, 0)
    pl.semaphore_wait(barrier, n - 1)

    def send(i, carry):
        pltpu.make_async_remote_copy(
            src_ref=in_ref, dst_ref=out_ref.at[me], send_sem=send_sem, recv_sem=recv_sem,
            device_id=(lax.rem(me + i, n),), device_id_type=MESH).start()
        return carry

    lax.fori_loop(1, n, send, 0)
    others = out_ref.at[pl.ds(0, n - 1)]
    drain = pltpu.make_async_remote_copy(
        src_ref=others, dst_ref=others, send_sem=send_sem, recv_sem=recv_sem,
        device_id=(me,), device_id_type=MESH)
    drain.wait_recv()
    drain.wait_send()
    out_ref[me] = in_ref[...]


def spread(block, n, cid):
    return pl.pallas_call(
        functools.partial(spread_kernel, n),
        out_shape=jax.ShapeDtypeStruct((n,) + block.shape, block.dtype),
        in_specs=[pl.BlockSpec(memory_space=pltpu.VMEM)],
        out_specs=pl.BlockSpec(memory_space=pltpu.VMEM),
        scratch_shapes=[pltpu.SemaphoreType.DMA, pltpu.SemaphoreType.DMA],
        compiler_params=pltpu.CompilerParams(collective_id=cid, has_side_effects=True),
        name=f'spread_{cid}',
    )(block)


def reduce_kernel(tile, steps, in_ref, out_ref, fresh, held, *scratch):
    got, (load_sem, send_sem, recv_sem, store_sem) = scratch[:steps], scratch[steps:]
    me = lax.axis_index('dp')
    core = lax.rem(me, 2)
    xb, yb = lax.rem(me // 2, 2), lax.rem(me // 4, 2)
    z0, z1 = lax.rem(me // 8, 2), lax.rem(me // 16, 2)
    def way(part):
        turn = lax.rem(part - (part + 2) // 4 + core, 2)
        one = (1 + turn, xb * (1 - turn) + yb * turn)
        two = (2 - turn, yb * (1 - turn) + xb * turn)
        plain = (one, two, (4, z0), (8, z1))[:steps - 1]
        turned = ((4, z0), (8, z1), one, two) if steps > 4 else ((4, z0), one, two)
        flip = (lax.rem(part, 4) + 3) // 4 * (1 - lax.rem(part, 4) // 2)
        return [(p + flip * (t - p), q + flip * (u - q)) for (p, q), (t, u) in zip(plain, turned)]

    def mate(step, part):
        if step == 0:
            return me + 1 - 2 * core
        weight, bit = way(part)[step - 1]
        return me + 2 * weight * (1 - 2 * bit)

    barrier = pltpu.get_barrier_semaphore()
    for step in range(steps):
        pl.semaphore_signal(barrier, inc=1, device_id=(mate(step, 0),), device_id_type=MESH)

    def piece(part):
        if tile[0] is None:
            return (slice(None), pl.ds(pl.multiple_of(part * tile[1], tile[1]), tile[1]))
        return (pl.ds(pl.multiple_of(part * tile[0], tile[0]), tile[0]),)

    def load(part):
        side = lax.rem(part, 2)
        return pltpu.make_async_copy(in_ref.at[(slice(None), slice(None)) + piece(part)], fresh.at[side], load_sem.at[side])

    load(0).start()
    load(1).start()
    pl.semaphore_wait(barrier, steps)

    def start_of(step, part, theirs):
        at = 0
        for k, (_, own) in enumerate(way(part)[:step]):
            bit = 1 - own if theirs and k == step - 1 else own
            at = at + bit * (1 << (steps - 2 - k))
        return at

    def send(step, part):
        if step == 0:
            group = got[0].shape[1] // 4
            for k in range(4):
                run = pl.ds(k * group, group)
                pltpu.make_async_remote_copy(
                    src_ref=fresh.at[lax.rem(part, 2), run, 1 - core], dst_ref=got[0].at[part, run],
                    send_sem=send_sem.at[0, part], recv_sem=recv_sem.at[0, part],
                    device_id=(mate(0, part),), device_id_type=MESH).start()
            return
        source = held.at[part, pl.ds(start_of(step, part, True), got[step].shape[1])]
        pltpu.make_async_remote_copy(
            src_ref=source, dst_ref=got[step].at[part], send_sem=send_sem.at[step, part],
            recv_sem=recv_sem.at[step, part], device_id=(mate(step, part),), device_id_type=MESH).start()

    def landed(step, part):
        return pltpu.make_async_remote_copy(
            src_ref=got[step].at[part], dst_ref=got[step].at[part],
            send_sem=send_sem.at[step, part], recv_sem=recv_sem.at[step, part],
            device_id=(mate(step, part),), device_id_type=MESH)

    def add(step, part):
        dims = way(part)
        start = start_of(step, part, False)

        def one(i, carry):
            if step == 0:
                at = 0
                for k, (weight, _) in enumerate(dims):
                    at = at + lax.rem(i // weight, 2) * (1 << (steps - 2 - k))
                held[part, at] = fresh[lax.rem(part, 2), i, core] + got[0][part, i]
            else:
                held[part, start + i] = held[part, start + i] + got[step][part, i]
            return carry
        lax.fori_loop(0, got[step].shape[1], one, 0)

    def store(part):
        return pltpu.make_async_copy(held.at[part, start_of(steps - 1, part, False)], out_ref.at[piece(part)],
                                     store_sem.at[part])

    def tick(t, carry):
        @pl.when(t < PARTS)
        def _():
            load(t).wait()
            send(0, t)

        for step in range(steps):
            part = t - 1 - step

            @pl.when((part >= 0) & (part < PARTS))
            def _():
                landed(step, part).wait_recv()
                add(step, part)
                if step < steps - 1:
                    send(step + 1, part)
                else:
                    store(part).start()
                if step == 0:
                    landed(0, part).wait_send()

                    @pl.when(part + 2 < PARTS)
                    def _():
                        load(part + 2).start()

        return carry

    lax.fori_loop(0, PARTS + steps, tick, 0)

    def finish(part, carry):
        for step in range(1, steps):
            landed(step, part).wait_send()
        store(part).wait()
        return carry

    lax.fori_loop(0, PARTS, finish, 0)


def reduce_scatter(x, n, cid):
    per, rest = x.shape[0] // n, x.shape[1:]
    if len(rest) == 2 or per // PARTS >= 8:
        tile, piece = (per // PARTS, None), (per // PARTS,) + rest
    else:
        tile, piece = (None, rest[0] // PARTS), (per, rest[0] // PARTS)
    steps = n.bit_length() - 1
    got = [pltpu.VMEM((PARTS, n >> (s + 1)) + piece, x.dtype) for s in range(steps)]
    size = x.size * x.dtype.itemsize
    return pl.pallas_call(
        functools.partial(reduce_kernel, tile, steps),
        out_shape=jax.ShapeDtypeStruct((per,) + rest, x.dtype),
        in_specs=[pl.BlockSpec(memory_space=pl.ANY)],
        out_specs=pl.BlockSpec(memory_space=pl.ANY),
        scratch_shapes=[pltpu.VMEM((2, n // 2, 2) + piece, x.dtype), pltpu.VMEM((PARTS, n // 2) + piece, x.dtype)] + got + [
            pltpu.SemaphoreType.DMA((2,)),
            pltpu.SemaphoreType.DMA((steps, PARTS)),
            pltpu.SemaphoreType.DMA((steps, PARTS)),
            pltpu.SemaphoreType.DMA((PARTS,)),
        ],
        compiler_params=pltpu.CompilerParams(collective_id=cid, has_side_effects=True,
                                             vmem_limit_bytes=min(size * 15 // 8 + 4 * 2**20, 67043328)),
        name=f'reduce_{cid}',
    )(x.reshape((n // 2, 2, per) + rest))


SLOT_BITS = 1024
OUT_ROWS = 256


def pick_kernel(n, count, rows_dev, keys, first, last, table, tgt_out, cand_out, buf, sems):
    base = lax.axis_index('dp') * rows_dev
    tok_dev = tgt_out.shape[1]

    def zero(i, carry):
        for side in range(2):
            buf[side, pl.ds(i * 32, 32)] = jnp.zeros((32,) + buf.shape[2:], buf.dtype)
        return carry

    lax.fori_loop(0, count // 32, zero, 0)

    def out_copies(j, side):
        return (pltpu.make_async_copy(buf.at[side, pl.ds(0, tok_dev)], tgt_out.at[j], sems.at[side, 0]),
                pltpu.make_async_copy(buf.at[side, pl.ds(tok_dev, count - tok_dev)], cand_out.at[j], sems.at[side, 1]))

    def per_dev(j, carry):
        side = lax.rem(j, 2)

        @pl.when(j >= 2)
        def _():
            for copy in out_copies(j - 2, side):
                copy.wait()

            def clear(i, c):
                buf[side, lax.rem(keys[(j - 2) * count + i], SLOT_BITS)] = jnp.zeros(buf.shape[2:], buf.dtype)
                return c

            lax.fori_loop(first[j - 2], last[j - 2], clear, 0)

        def one(i, c):
            key = keys[j * count + i]
            buf[side, lax.rem(key, SLOT_BITS)] = table[key // SLOT_BITS - base]
            return c

        lax.fori_loop(first[j], last[j], one, 0)
        for copy in out_copies(j, side):
            copy.start()
        return carry

    lax.fori_loop(0, n, per_dev, 0)
    for copy in out_copies(n - 2, 0) + out_copies(n - 1, 1):
        copy.wait()


def pick_rows(table3, keys, first, last, n, count, tok_dev):
    smem = pl.BlockSpec(memory_space=pltpu.SMEM)
    anywhere = pl.BlockSpec(memory_space=pl.ANY)
    tail = table3.shape[1:]
    return pl.pallas_call(
        functools.partial(pick_kernel, n, count, table3.shape[0]),
        out_shape=(jax.ShapeDtypeStruct((n, tok_dev) + tail, table3.dtype),
                   jax.ShapeDtypeStruct((n, count - tok_dev) + tail, table3.dtype)),
        in_specs=[smem, smem, smem, pl.BlockSpec(memory_space=pltpu.VMEM)],
        out_specs=(anywhere, anywhere),
        scratch_shapes=[pltpu.VMEM((2, count) + tail, table3.dtype), pltpu.SemaphoreType.DMA((2, 2))],
        compiler_params=pltpu.CompilerParams(vmem_limit_bytes=24 * 2**20),
        name='pick_rows',
    )(keys, first, last, table3)


def table_kernel(n, count, tok_dev, rows_dev, lane, keys, first, last, scale, query, cand, out_ref, acc):
    step = pl.program_id(0)
    base = lax.axis_index('dp') * rows_dev

    @pl.when(step == 0)
    def _():
        def zero(i, carry):
            acc[pl.ds(i * 64, 64)] = jnp.zeros((64,) + acc.shape[1:], jnp.float32)
            return carry

        lax.fori_loop(0, rows_dev // 64, zero, 0)

    @pl.when(step < n)
    def _():
        def one(i, carry):
            key = keys[step * count + i]
            at = key // SLOT_BITS - base
            slot = lax.rem(key, SLOT_BITS)

            @pl.when(slot < tok_dev)
            def _():
                acc[at] = acc[at] + scale[step * tok_dev + slot] * query[slot].astype(jnp.float32)

            @pl.when(slot >= tok_dev)
            def _():
                acc[at] = acc[at] + cand[slot - tok_dev]

            return carry

        lax.fori_loop(first[step], last[step], one, 0)

    @pl.when(step >= n)
    def _():
        for j in range(acc.shape[1]):
            out_ref[:, j * lane:(j + 1) * lane] = acc[pl.ds((step - n) * OUT_ROWS, OUT_ROWS), j, :]


def table_grad(keys, first, last, scale, query, cand, rows_dev, n, count):
    tok_dev, cand_dev = query.shape[0] // n, cand.shape[0] // n
    sub, lane = query.shape[1:]
    smem = pl.BlockSpec(memory_space=pltpu.SMEM)
    size = 4 * rows_dev * sub * lane
    return pl.pallas_call(
        functools.partial(table_kernel, n, count, tok_dev, rows_dev, lane),
        grid=(n + rows_dev // OUT_ROWS,),
        out_shape=jax.ShapeDtypeStruct((rows_dev, sub * lane), jnp.float32),
        in_specs=[smem, smem, smem, smem,
                  pl.BlockSpec((tok_dev, sub, lane), lambda i: (jnp.minimum(i, n - 1), 0, 0)),
                  pl.BlockSpec((cand_dev, sub, lane), lambda i: (jnp.minimum(i, n - 1), 0, 0))],
        out_specs=pl.BlockSpec((OUT_ROWS, sub * lane), lambda i: (jnp.maximum(i - n, 0), 0)),
        scratch_shapes=[pltpu.VMEM((rows_dev, sub, lane), jnp.float32)],
        cost_estimate=pl.CostEstimate(flops=30_000_000_000, bytes_accessed=4 * size, transcendentals=0),
        compiler_params=pltpu.CompilerParams(vmem_limit_bytes=size + 12 * 2**20),
        name='table_grad',
    )(keys, first, last, scale, query, cand)


def outer_kernel(left, right, out_ref):
    out_ref[...] = jnp.dot(left[...], right[...], preferred_element_type=jnp.float32)


def outer(left, right):
    rows, depth = left.shape
    cols = right.shape[1]
    high, wide = rows, cols // 8
    return pl.pallas_call(
        outer_kernel,
        grid=(rows // high, cols // wide),
        out_shape=jax.ShapeDtypeStruct((rows, cols), jnp.float32),
        in_specs=[pl.BlockSpec((high, depth), lambda i, j: (i, 0)), pl.BlockSpec((depth, wide), lambda i, j: (0, j))],
        out_specs=pl.BlockSpec((high, wide), lambda i, j: (i, j)),
        cost_estimate=pl.CostEstimate(flops=2 * rows * cols * depth, bytes_accessed=4 * rows * cols, transcendentals=0),
        compiler_params=pltpu.CompilerParams(vmem_limit_bytes=16 * 2**20),
        name='outer',
    )(left, right)


def carry_kernel(in_ref, out_ref):
    out_ref[...] = in_ref[...]


def carry_over(x):
    rows, cols = x.shape
    spec = pl.BlockSpec((rows // 8, cols), lambda i: (i, 0))
    return pl.pallas_call(
        carry_kernel, grid=(8,), out_shape=jax.ShapeDtypeStruct(x.shape, x.dtype), in_specs=[spec], out_specs=spec,
        cost_estimate=pl.CostEstimate(flops=x.size, bytes_accessed=8 * x.size, transcendentals=0),
        compiler_params=pltpu.CompilerParams(vmem_limit_bytes=16 * 2**20), name='carry_over')(x)


def solution(mesh):
    n = mesh.shape['dp']

    def local_step(x_blk, w_one, w_two, table_blk, cand_ids, cand_logq, y_blk):
        tok_dev = x_blk.shape[0]
        rows_dev, emb_dim = table_blk.shape
        total_tok = tok_dev * n
        cand_dev = cand_ids.shape[0] // n
        count = tok_dev + cand_dev
        lane = 128
        sub = emb_dim // lane
        me = lax.axis_index('dp')

        slots = jnp.arange(count, dtype=jnp.int32)
        wants = jnp.concatenate([y_blk, lax.dynamic_slice(cand_ids, (me * cand_dev,), (cand_dev,))]) * SLOT_BITS + slots
        rank = jnp.sum((wants[None, :] < wants[:, None]).astype(jnp.int32), axis=1)
        sorted_own = jnp.sum(jnp.where(rank[:, None] == slots[None, :], wants[:, None], 0), axis=0)
        block = jnp.pad(sorted_own, (0, (-count) % (8 * lane))).reshape(-1, lane)
        everyone = spread(block, n, 0).reshape(n, -1)[:, :count]
        first = jnp.sum((everyone < me * rows_dev * SLOT_BITS).astype(jnp.int32), axis=1)
        last = jnp.sum((everyone - me * rows_dev * SLOT_BITS < rows_dev * SLOT_BITS).astype(jnp.int32), axis=1)
        keys = everyone.reshape(-1)

        tgt_part, cand_part = pick_rows(table_blk.reshape(rows_dev, sub, lane), keys, first, last, n, count, tok_dev)
        own_cand = reduce_scatter(cand_part.reshape(n * cand_dev, sub, lane), n, 5).reshape(cand_dev, emb_dim)
        cand_rows = lax.all_gather(own_cand, 'dp', tiled=True)

        x_flip = lax.optimization_barrier(x_blk.T)
        pre_act = jnp.dot(x_blk, w_one, preferred_element_type=jnp.float32).astype(jnp.bfloat16)
        act_val, gelu_back = jax.vjp(jax.nn.gelu, pre_act.astype(jnp.float32))
        hidden_act = act_val.astype(jnp.bfloat16)
        query_vec = jnp.dot(hidden_act, w_two, preferred_element_type=jnp.float32).astype(jnp.bfloat16)
        query_all = lax.all_gather(query_vec.reshape(tok_dev, sub, lane), 'dp', tiled=True)
        tgt_part, query_vec = lax.optimization_barrier((tgt_part, query_vec))
        tgt_rows = reduce_scatter(tgt_part.reshape(n * tok_dev, sub, lane), n, 6).reshape(tok_dev, emb_dim)

        z_tgt = jnp.einsum('td,td->t', query_vec, tgt_rows, preferred_element_type=jnp.float32)
        z_cand = jnp.einsum('td,sd->ts', query_vec, cand_rows, preferred_element_type=jnp.float32) - cand_logq[None, :]
        z_cand = jnp.where(y_blk[:, None] == cand_ids[None, :], -1e9, z_cand)
        peak_val = jnp.maximum(jnp.max(z_cand, axis=1), z_tgt)
        exp_total = jnp.exp(z_tgt - peak_val) + jnp.sum(jnp.exp(z_cand - peak_val[:, None]), axis=1)
        log_norm = peak_val + jnp.log(exp_total)
        loss_part = jnp.sum(log_norm - z_tgt)
        dz_tgt = (jnp.exp(z_tgt - log_norm) - 1.0) / total_tok
        dz_cand = (jnp.exp(z_cand - log_norm[:, None]) / total_tok).astype(jnp.bfloat16)
        d_query = (dz_tgt[:, None] * tgt_rows.astype(jnp.float32)
                   + jnp.dot(dz_cand, cand_rows, preferred_element_type=jnp.float32)).astype(jnp.bfloat16)

        note = jnp.concatenate([dz_tgt, jnp.broadcast_to(loss_part, (8 * lane - tok_dev,))]).reshape(8, lane)
        notes = spread(note, n, 4).reshape(n, 8 * lane)
        loss_val = jnp.sum(notes[:, tok_dev]) / total_tok
        part_cand = jnp.einsum('ts,td->sd', dz_cand, query_vec, preferred_element_type=jnp.float32)
        own_cand_grad = reduce_scatter(part_cand, n, 1)
        sent_cand, query_all = lax.optimization_barrier((own_cand_grad.reshape(cand_dev, sub, lane), query_all))
        cand_grad = lax.all_gather(sent_cand, 'dp', tiled=True)

        part_two = jnp.einsum('tf,td->fd', hidden_act, d_query, preferred_element_type=jnp.float32)
        part_two, own_cand_grad = lax.optimization_barrier((part_two, own_cand_grad))
        own_two = reduce_scatter(part_two, n, 2)
        sent_two, cand_grad = lax.optimization_barrier((own_two, cand_grad))
        grad_two = lax.all_gather(sent_two, 'dp', tiled=True)

        d_act = jnp.einsum('td,fd->tf', d_query, w_two, preferred_element_type=jnp.float32)
        d_pre = gelu_back(d_act.astype(jnp.bfloat16).astype(jnp.float32))[0].astype(jnp.bfloat16)
        part_one = outer(x_flip, d_pre)
        part_one, own_two = lax.optimization_barrier((part_one, own_two))
        own_one = reduce_scatter(part_one, n, 3)
        sent_one, grad_two = lax.optimization_barrier((own_one, grad_two))
        grad_one = carry_over(lax.all_gather(sent_one, 'dp', tiled=True))
        grad_two = carry_over(grad_two)

        grad_table = table_grad(keys, first, last, notes[:, :tok_dev].reshape(-1), query_all, cand_grad, rows_dev, n, count)
        return loss_val, grad_table, grad_one, grad_two

    return jax.shard_map(local_step, mesh=mesh,
                         in_specs=(P('dp', None), P(), P(), P('dp', None), P(), P(), P('dp')),
                         out_specs=(P(), P('dp', None), P(), P()), check_vma=False)
```
